32 devices in a mesh: dp: 16 (over z, y, x), mp: 2 (over core).
Axes of the slice: x: 2, y: 2, z: 4, core: 2. Of those that a mesh axis runs over, the one named last changes fastest.
Arguments:
- tokens: bfloat16 [32768, 768], P(('dp', 'mp')), may hold values from -6 to 6
- w_query: bfloat16 [768, 768], P('dp', 'mp'), may hold values from -0.625 to 0.625
- w_key: bfloat16 [768, 768], P('dp', 'mp'), may hold values from -0.625 to 0.625
- w_value: bfloat16 [768, 768], P('dp', 'mp'), may hold values from -0.21875 to 0.21875
- value_taps: float32 [12, 33], P('mp'), may hold values from -0.3 to 0.3
- w_output: bfloat16 [768, 768], P(None, ('dp', 'mp')), may hold values from -0.875 to 0.875
- first_gain: bfloat16 [768], P(('dp', 'mp')), may hold values from 0.25 to 1.75
- first_bias: bfloat16 [768], P(('dp', 'mp')), may hold values from -1.5 to 1.5
- w_expand: bfloat16 [768, 3072], P('dp', 'mp'), may hold values from -0.21875 to 0.21875
- w_shrink: bfloat16 [3072, 768], P('mp', 'dp'), may hold values from -0.21875 to 0.21875
- second_gain: bfloat16 [768], P(('dp', 'mp')), may hold values from 0.25 to 1.75
- second_bias: bfloat16 [768], P(('dp', 'mp')), may hold values from -1.5 to 1.5
- doc_lengths: int32 [32], replicated, may hold values from 256 to 1024, as said below
- out_grad: bfloat16 [32768, 768], P(('dp', 'mp')), may hold values from -6 to 6
Outputs:
- layer_out: bfloat16 [32768, 768], P(('dp', 'mp'))
- tokens_grad: float32 [32768, 768], P(('dp', 'mp'))
- query_grad: float32 [768, 768], P('dp', 'mp')
- key_grad: float32 [768, 768], P('dp', 'mp')
- value_grad: float32 [768, 768], P('dp', 'mp')
- taps_grad: float32 [12, 33], P('mp')
- output_grad: float32 [768, 768], P(None, ('dp', 'mp'))
- first_gain_grad: float32 [768], P(('dp', 'mp'))
- first_bias_grad: float32 [768], P(('dp', 'mp'))
- expand_grad: float32 [768, 3072], P('dp', 'mp')
- shrink_grad: float32 [3072, 768], P('mp', 'dp')
- second_gain_grad: float32 [768], P(('dp', 'mp'))
- second_bias_grad: float32 [768], P(('dp', 'mp'))
The draws below stay inside these ranges and needn't reach their ends.
Inputs may be any that keep to these rules, and one draw needn't show every extreme that they name: Document i occupies the first doc_lengths[i] positions of slot i of 1024 positions; the rest is padding. In every draw some document fills its whole slot.
All inputs are finite; a program needn't handle non-finite values.
Results may differ from the reference program's by a relative error of at most 0.018.
The reference program's roundings to bfloat16 on the way count: a program that leaves them out, or rounds other values in their place, can miss the bound.
Values may be sent and summed in bfloat16 or wider, within the bound.
A program may use at most 320 MiB of HBM per device.

```python
import jax
import jax.numpy as jnp
from jax import lax

D = 768
HEADS = 12
HEAD_DIM = 64
FF = 3072
LANDMARKS = 64
KERNEL = 33
PINV_STEPS = 6
SLOT = 1024
DOCS = 32
TOKENS = 32768
N_DP = 16
N_MP = 2


def draw_doc_lengths(key, part):
    lowest = max(LANDMARKS, SLOT // 4)
    drawn = jax.random.randint(key, (DOCS,), lowest, SLOT + 1)
    chosen = jax.random.randint(jax.random.fold_in(key, 11), (), 0, DOCS)
    return drawn.at[chosen].set(SLOT).astype(jnp.int32)


def block_scale(key, dims, shards, smallest, high):
    loudness, own = 1.0, jax.random.fold_in(key, 6)
    for position, shards_of in shards:
        draws = jnp.exp(jax.random.uniform(jax.random.fold_in(own, position), (shards_of,), jnp.float32, smallest / len(shards), high / len(shards)))
        loudness = loudness * jnp.repeat(draws, dims[position] // shards_of).reshape([-1 if axis == position else 1 for axis in range(len(dims))])
    return loudness


def noise(stream_key, extent, deviation, most, split=(), kind=jnp.bfloat16):
    values = jax.random.normal(stream_key, extent, jnp.float32) * deviation
    if len(split) > 0:
        values = block_scale(stream_key, extent, split, -0.22, 0.18) * values
    return jnp.clip(values, min=-most, max=most).astype(kind)


def setup_inputs(seed: int = 0) -> dict:
    seeds = jax.random.split(jax.random.key(seed), 15)
    tokens = noise(seeds[0], (TOKENS, D), 1.0, 6.0, ((0, 32),))
    w_query = noise(seeds[1], (D, D), (D // 8) ** -0.5, 0.625, ((0, 16), (1, 2)))
    w_key = noise(seeds[2], (D, D), (D // 8) ** -0.5, 0.625, ((0, 16), (1, 2)))
    w_value = noise(seeds[3], (D, D), D ** -0.5, 0.21875, ((0, 16), (1, 2)))
    value_taps = noise(seeds[4], (HEADS, KERNEL), 0.05, 0.3, ((0, 2),), jnp.float32)
    w_output = noise(seeds[5], (D, D), (D // 16) ** -0.5, 0.875, ((1, 32),))
    first_gain = jnp.clip(1.0 + 0.15 * jax.random.normal(seeds[6], (D,), jnp.float32), 0.25, 1.75).astype(jnp.bfloat16)
    first_bias = noise(seeds[7], (D,), 0.3, 1.5, ((0, 32),))
    w_expand = noise(seeds[8], (D, FF), D ** -0.5, 0.21875, ((0, 16), (1, 2)))
    w_shrink = noise(seeds[9], (FF, D), (FF // 4) ** -0.5, 0.21875, ((0, 2), (1, 16)))
    second_gain = jnp.clip(1.0 + 0.15 * jax.random.normal(seeds[10], (D,), jnp.float32), 0.25, 1.75).astype(jnp.bfloat16)
    second_bias = noise(seeds[11], (D,), 0.3, 1.5, ((0, 32),))
    doc_lengths = draw_doc_lengths(jax.random.fold_in(seeds[14], 71), 0)
    out_grad = noise(seeds[13], (TOKENS, D), 1.0, 6.0, ((0, 32),))
    return dict(tokens=tokens, w_query=w_query, w_key=w_key, w_value=w_value, value_taps=value_taps, w_output=w_output, first_gain=first_gain, first_bias=first_bias, w_expand=w_expand, w_shrink=w_shrink, second_gain=second_gain, second_bias=second_bias, doc_lengths=doc_lengths, out_grad=out_grad)


HIGH = lax.Precision.HIGHEST

@jax.custom_vjp
def low(v):
    return lax.optimization_barrier(v.astype(jnp.bfloat16)).astype(jnp.float32)

@jax.custom_vjp
def low_back(v):
    return v

def low_keep(v):
    return (low(v), None)

def low_pass(kept, grad):
    return (grad,)

def back_keep(v):
    return (v, None)

def back_low(kept, grad):
    return (low(grad),)
low.defvjp(low_keep, low_pass)
low_back.defvjp(back_keep, back_low)

def layer_norm(values, gain, bias):
    middle = lax.optimization_barrier(jnp.mean(values, axis=-1, keepdims=True))
    centered = values - middle
    variance = lax.optimization_barrier(jnp.mean(centered * centered, axis=-1, keepdims=True))
    return centered * lax.rsqrt(variance + 1e-05) * gain + bias

def inverse_estimate(matrix):
    widest = lax.optimization_barrier(jnp.max(lax.optimization_barrier(jnp.sum(matrix, axis=-2)), axis=-1))
    current = jnp.swapaxes(matrix, -1, -2) / widest[:, None, None]
    identity = jnp.eye(matrix.shape[-1], dtype=jnp.float32)[None]
    for step in range(PINV_STEPS):
        product = jnp.einsum('hij,hjk->hik', matrix, current, precision=HIGH)
        inner_term = 7.0 * identity - product
        inner_term = 15.0 * identity - jnp.einsum('hij,hjk->hik', product, inner_term, precision=HIGH)
        inner_term = 13.0 * identity - jnp.einsum('hij,hjk->hik', product, inner_term, precision=HIGH)
        current = 0.25 * jnp.einsum('hij,hjk->hik', current, inner_term, precision=HIGH)
    return current

def nystrom(query, keys, values, taps, length):
    positions = jnp.arange(SLOT, dtype=jnp.int32)
    valid = positions < length
    weight = valid.astype(jnp.float32)
    segment = positions * LANDMARKS // length
    member = ((segment[None, :] == jnp.arange(LANDMARKS, dtype=jnp.int32)[:, None]) & valid[None, :]).astype(jnp.float32)
    member = member / lax.optimization_barrier(jnp.sum(member, axis=1, keepdims=True))
    mark_query = jnp.einsum('js,shd->hjd', member, query, precision=HIGH)
    mark_keys = jnp.einsum('js,shd->hjd', member, keys, precision=HIGH)
    scale = HEAD_DIM ** (-0.5)
    first = jax.nn.softmax(jnp.einsum('shd,hjd->hsj', query, mark_keys, precision=HIGH) * scale, axis=-1)
    second = jax.nn.softmax(jnp.einsum('hid,hjd->hij', mark_query, mark_keys, precision=HIGH) * scale, axis=-1)
    third_scores = jnp.einsum('hjd,shd->hjs', mark_query, keys, precision=HIGH) * scale
    third = jax.nn.softmax(jnp.where(valid[None, None, :], third_scores, -1e+30), axis=-1)
    inverse = inverse_estimate(second)
    summary = jnp.einsum('hjs,shd->hjd', third, values, precision=HIGH)
    carried = jnp.einsum('hij,hjd->hid', inverse, summary, precision=HIGH)
    mixed = jnp.einsum('hsj,hjd->shd', first, carried, precision=HIGH)
    radius = KERNEL // 2
    padded = jnp.pad(values * weight[:, None, None], ((radius, radius), (0, 0), (0, 0)))
    for index in range(KERNEL):
        mixed = mixed + taps[:, index][None, :, None] * padded[index:index + SLOT]
    mixed = mixed * weight[:, None, None]
    return mixed.reshape(SLOT, query.shape[1] * HEAD_DIM)

def group_layer(weights, tokens, lengths):
    w_q, w_k, w_v, taps, w_o, gain_one, bias_one, w_e, w_s, gain_two, bias_two = weights
    rows = tokens.shape[0]

    def project(matrix):
        result = low_back(low(jnp.dot(tokens, matrix, precision=HIGH)))
        return result.reshape(N_MP, SLOT, HEADS, HEAD_DIM)
    attended = jax.vmap(nystrom, in_axes=(0, 0, 0, None, 0))(project(w_q), project(w_k), project(w_v), taps, lengths)
    attended = low_back(low(attended.reshape(rows, D)))
    projected = low_back(jnp.dot(attended, w_o, precision=HIGH))
    first_out = layer_norm(tokens + projected, gain_one, bias_one)
    pre = low_back(jnp.dot(low(first_out), w_e, precision=HIGH))
    active = low(jax.nn.gelu(pre, approximate=False))
    branch = low_back(jnp.dot(active, w_s, precision=HIGH))
    return layer_norm(first_out + branch, gain_two, bias_two)

def reference(tokens, w_query, w_key, w_value, value_taps, w_output, first_gain, first_bias, w_expand, w_shrink, second_gain, second_bias, doc_lengths, out_grad):
    floats = [a.astype(jnp.float32) for a in (tokens, w_query, w_key, w_value, value_taps, w_output, first_gain, first_bias, w_expand, w_shrink, second_gain, second_bias)]
    pairs = doc_lengths.astype(jnp.int32).reshape(N_DP, N_MP)

    def forward(inputs, *weights):
        grouped = inputs.reshape(N_DP, N_MP * SLOT, D)
        stepper = jax.checkpoint(group_layer)

        def visit(carry, item):
            return (carry, stepper(weights, item[0], item[1]))
        unused, outs = lax.scan(visit, jnp.float32(0.0), (grouped, pairs))
        return outs.reshape(TOKENS, D)
    result, back = jax.vjp(forward, *floats)
    grads = back(out_grad.astype(jnp.float32))
    return (result.astype(jnp.bfloat16), grads[0], grads[1], grads[2], grads[3], grads[4], grads[5], grads[6], grads[7], grads[8], grads[9], grads[10], grads[11])
```

```python
import jax
import jax.numpy as jnp
from jax import lax
from jax.sharding import PartitionSpec as P

HEAD_DIM = 64
LANDMARKS = 64
KERNEL = 33
PINV_STEPS = 6
HIGH = lax.Precision.HIGHEST


def ahead(left, right):
    return jnp.dot(left, right, preferred_element_type=jnp.float32)


def against(left, right):
    return lax.dot_general(
        left, right, (((1,), (1,)), ((), ())), preferred_element_type=jnp.float32
    )


def across(left, right):
    return lax.dot_general(
        left, right, (((0,), (0,)), ((), ())), preferred_element_type=jnp.float32
    )


def low(values):
    return values.astype(jnp.bfloat16)


def wide(values):
    return values.astype(jnp.float32)


def layer_norm(values, gain, bias):
    middle = jnp.mean(values, axis=-1, keepdims=True)
    centered = values - middle
    variance = jnp.mean(centered * centered, axis=-1, keepdims=True)
    return centered * lax.rsqrt(variance + 1e-05) * gain + bias


def exact_gelu(values):
    return jax.nn.gelu(values, approximate=False)


def inverse_estimate(matrix):
    widest = jnp.max(jnp.sum(matrix, axis=-2), axis=-1)
    current = jnp.swapaxes(matrix, -1, -2) / widest[:, None, None]
    identity = jnp.eye(matrix.shape[-1], dtype=jnp.float32)[None]
    for step in range(PINV_STEPS):
        product = jnp.einsum("hij,hjk->hik", matrix, current, precision=HIGH)
        inner_term = 7.0 * identity - product
        inner_term = 15.0 * identity - jnp.einsum(
            "hij,hjk->hik", product, inner_term, precision=HIGH
        )
        inner_term = 13.0 * identity - jnp.einsum(
            "hij,hjk->hik", product, inner_term, precision=HIGH
        )
        current = 0.25 * jnp.einsum("hij,hjk->hik", current, inner_term, precision=HIGH)
    return current


def nystrom(query, keys, values, taps, length):
    slots = query.shape[0]
    positions = jnp.arange(slots, dtype=jnp.int32)
    valid = positions < length
    weight = valid.astype(jnp.float32)
    segment = positions * LANDMARKS // length
    member = (
        (segment[None, :] == jnp.arange(LANDMARKS, dtype=jnp.int32)[:, None]) & valid[None, :]
    ).astype(jnp.float32)
    member = member / jnp.sum(member, axis=1, keepdims=True)
    mark_query = jnp.einsum("js,shd->hjd", member, query, precision=HIGH)
    mark_keys = jnp.einsum("js,shd->hjd", member, keys, precision=HIGH)
    scale = HEAD_DIM ** (-0.5)
    first = jax.nn.softmax(
        jnp.einsum("shd,hjd->hsj", query, mark_keys, precision=HIGH) * scale, axis=-1
    )
    second = jax.nn.softmax(
        jnp.einsum("hid,hjd->hij", mark_query, mark_keys, precision=HIGH) * scale, axis=-1
    )
    third_scores = jnp.einsum("hjd,shd->hjs", mark_query, keys, precision=HIGH) * scale
    third = jax.nn.softmax(jnp.where(valid[None, None, :], third_scores, -1e30), axis=-1)
    inverse = inverse_estimate(second)
    summary = jnp.einsum("hjs,shd->hjd", third, values, precision=HIGH)
    carried = jnp.einsum("hij,hjd->hid", inverse, summary, precision=HIGH)
    mixed = jnp.einsum("hsj,hjd->shd", first, carried, precision=HIGH)
    radius = KERNEL // 2
    padded = jnp.pad(values * weight[:, None, None], ((radius, radius), (0, 0), (0, 0)))
    for index in range(KERNEL):
        mixed = mixed + taps[:, index][None, :, None] * padded[index : index + slots]
    mixed = mixed * weight[:, None, None]
    return mixed.reshape(slots, query.shape[1] * HEAD_DIM)


def bits_of(size):
    return max(size - 1, 0).bit_length()


def flip(values, bit):
    size = lax.axis_size("dp")
    return lax.ppermute(values, "dp", [(i, i ^ (1 << bit)) for i in range(size)])


def partner(values):
    size = lax.axis_size("mp")
    return lax.ppermute(values, "mp", [(i, (i + 1) % size) for i in range(size)])


def spread_small(values):
    group = lax.axis_index("dp")
    values = values[:, None, :]
    for bit in range(bits_of(lax.axis_size("dp"))):
        other = flip(values, bit)
        upper = ((group >> bit) & 1) == 1
        values = jnp.where(
            upper,
            jnp.concatenate([other, values], axis=1),
            jnp.concatenate([values, other], axis=1),
        )
    return values.reshape(values.shape[0], -1)


def sum_all(values):
    for bit in range(bits_of(lax.axis_size("dp"))):
        values = values + flip(values, bit)
    return values


def fold(blocks, orders, kind):
    count = bits_of(lax.axis_size("dp"))
    group = lax.axis_index("dp")
    columns = blocks.shape[2]
    edges = [round(columns / 128 * i / len(orders)) * 128 for i in range(len(orders))] + [columns]
    pieces = []
    for color, order in enumerate(orders):
        if edges[color] == edges[color + 1]:
            continue
        part = blocks[:, :, edges[color] : edges[color + 1]]
        part = part.reshape((2,) * count + part.shape[1:])
        left = list(range(count))[::-1]
        for place, bit in enumerate(order):
            axis = left.index(bit)
            mine = (group >> bit) & 1
            keep = lax.dynamic_index_in_dim(part, mine, axis, keepdims=False)
            send = lax.dynamic_index_in_dim(part, 1 - mine, axis, keepdims=False)
            part = wide(keep) + wide(flip(send.astype(kind), bit))
            if place + 1 < count:
                part = part.astype(kind)
            left.pop(axis)
        pieces.append(part)
    return jnp.concatenate(pieces, axis=1) if len(pieces) > 1 else pieces[0]


def color_orders():
    count = bits_of(lax.axis_size("dp"))
    base = list(range(count))
    return [base, base[1:] + base[:1], base[2:] + base[:2]]


def on_device(
    tokens,
    w_query,
    w_key,
    w_value,
    value_taps,
    w_output,
    first_gain,
    first_bias,
    w_expand,
    w_shrink,
    second_gain,
    second_bias,
    doc_lengths,
    out_grad,
):
    parts = lax.axis_size("mp")
    groups = lax.axis_size("dp")
    group = lax.axis_index("dp")
    core = lax.axis_index("mp")
    slots, width = tokens.shape
    half = w_query.shape[1]
    hidden_half = w_expand.shape[1]
    rows = w_query.shape[0]
    length = lax.dynamic_index_in_dim(doc_lengths, group * parts + core, 0, keepdims=False)

    def in_core_order(own, other, axis):
        return jnp.where(
            core == 0,
            jnp.concatenate([own, other], axis=axis),
            jnp.concatenate([other, own], axis=axis),
        )

    output_t = w_output.T
    mine_cols = lax.dynamic_slice_in_dim(output_t, core * half, half, 1)
    their_cols = lax.dynamic_slice_in_dim(output_t, (1 - core) * half, half, 1)
    output_block = in_core_order(mine_cols, partner(their_cols), 0)
    head_block = jnp.concatenate([w_query, w_key, w_value, output_block], axis=1)
    hidden_block = jnp.concatenate([w_expand, w_shrink.T], axis=1)
    head_own = lax.all_gather(head_block, "dp", axis=0, tiled=True)
    head_other = partner(head_own)
    hidden_own = lax.all_gather(hidden_block, "dp", axis=0, tiled=True)
    hidden_other = partner(hidden_own)
    norms = jnp.stack([first_gain, first_bias, second_gain, second_bias])
    norms = in_core_order(norms, partner(norms), 1)
    gain_one, bias_one, gain_two, bias_two = wide(spread_small(norms))
    taps = jnp.concatenate([value_taps, partner(value_taps)], axis=0)

    def part_of(block, index, size):
        return block[:, index * size : (index + 1) * size]

    def both(index):
        return part_of(head_own, index, half), part_of(head_other, index, half)

    q_own, q_oth = both(0)
    k_own, k_oth = both(1)
    v_own, v_oth = both(2)
    o_own, o_oth = both(3)
    e_own, s_own = part_of(hidden_own, 0, hidden_half), part_of(hidden_own, 1, hidden_half)
    e_oth, s_oth = part_of(hidden_other, 0, hidden_half), part_of(hidden_other, 1, hidden_half)

    def project(own, oth):
        return jnp.concatenate([low(ahead(tokens, own)), low(ahead(tokens, oth))], axis=1)

    query_low, keys_low, values_low = project(q_own, q_oth), project(k_own, k_oth), project(v_own, v_oth)

    def attention_core(query, keys, values, taps):
        shape = (slots, width // HEAD_DIM, HEAD_DIM)
        return nystrom(
            query.reshape(shape), keys.reshape(shape), values.reshape(shape), taps, length
        )

    attended, core_back = jax.vjp(
        attention_core, wide(query_low), wide(keys_low), wide(values_low), taps
    )
    attended = low(attended)
    att_own, att_oth = attended[:, :half], attended[:, half:]
    projected = against(att_own, o_own) + against(att_oth, o_oth)
    first_out, first_back = jax.vjp(layer_norm, wide(tokens) + projected, gain_one, bias_one)
    hidden_in = low(first_out)
    act_own, gelu_own = jax.vjp(exact_gelu, ahead(hidden_in, e_own))
    act_oth, gelu_oth = jax.vjp(exact_gelu, ahead(hidden_in, e_oth))
    act_own, act_oth = low(act_own), low(act_oth)
    branch = against(act_own, s_own) + against(act_oth, s_oth)
    result, second_back = jax.vjp(layer_norm, first_out + branch, gain_two, bias_two)
    layer_out = low(result)
    d_second_in, gain_two_grad, bias_two_grad = second_back(wide(out_grad))
    d_branch = low(d_second_in)
    (d_pre_oth,) = gelu_oth(ahead(d_branch, s_oth))
    d_pre_oth = low(d_pre_oth)
    shrink_send = low(across(d_branch, act_oth))
    expand_send = low(across(hidden_in, d_pre_oth))
    shrink_got, expand_got = partner(shrink_send), partner(expand_send)
    (d_pre_own,) = gelu_own(ahead(d_branch, s_own))
    d_pre_own = low(d_pre_own)
    shrink_sum = low(across(d_branch, act_own) + wide(shrink_got))
    expand_sum = low(across(hidden_in, d_pre_own) + wide(expand_got))
    orders = color_orders()

    def blocks(values):
        return values.reshape(groups, rows, values.shape[1])

    shrink_grad = fold(blocks(shrink_sum), orders, jnp.bfloat16).T
    expand_grad = fold(blocks(expand_sum), orders, jnp.bfloat16)
    d_hidden = against(d_pre_own, e_own) + against(d_pre_oth, e_oth)
    d_first_in, gain_one_grad, bias_one_grad = first_back(d_second_in + d_hidden)
    d_projected = low(d_first_in)
    d_attended = jnp.concatenate([low(ahead(d_projected, o_own)), low(ahead(d_projected, o_oth))], axis=1)
    norm_grads = jnp.stack([gain_one_grad, bias_one_grad, gain_two_grad, bias_two_grad])
    norm_grads = norm_grads + partner(norm_grads)
    norm_grads = fold(
        norm_grads.reshape(4, groups, rows).swapaxes(0, 1), orders[:1], jnp.float32
    )
    norm_grads = lax.dynamic_slice_in_dim(norm_grads, core * (rows // parts), rows // parts, 1)
    d_query, d_keys, d_values, taps_grad = core_back(wide(d_attended))
    d_query, d_keys, d_values = low(d_query), low(d_keys), low(d_values)
    taps_grad = sum_all(taps_grad[: taps_grad.shape[0] // 2] + partner(taps_grad[taps_grad.shape[0] // 2 :]))

    def owned(values):
        return values[:, :half]

    def others(values):
        return values[:, half:]

    head_send = low(
        jnp.concatenate(
            [
                across(tokens, others(d_query)),
                across(tokens, others(d_keys)),
                across(tokens, others(d_values)),
                across(d_projected, att_oth),
            ],
            axis=1,
        )
    )
    head_got = partner(head_send)
    head_sum = low(
        jnp.concatenate(
            [
                across(tokens, owned(d_query)),
                across(tokens, owned(d_keys)),
                across(tokens, owned(d_values)),
                across(d_projected, att_own),
            ],
            axis=1,
        )
        + wide(head_got)
    )
    head_grads = fold(blocks(head_sum), orders, jnp.bfloat16)
    tokens_grad = d_first_in + (
        against(owned(d_query), q_own)
        + against(others(d_query), q_oth)
        + against(owned(d_keys), k_own)
        + against(others(d_keys), k_oth)
        + against(owned(d_values), v_own)
        + against(others(d_values), v_oth)
    )
    query_grad, key_grad, value_grad, output_part = (
        head_grads[:, i * half : (i + 1) * half] for i in range(4)
    )
    keep_rows = lax.dynamic_slice_in_dim(output_part, core * (rows // parts), rows // parts, 0)
    send_rows = lax.dynamic_slice_in_dim(output_part, (1 - core) * (rows // parts), rows // parts, 0)
    output_grad = in_core_order(keep_rows, partner(send_rows), 1).T
    return (
        layer_out,
        tokens_grad,
        query_grad,
        key_grad,
        value_grad,
        taps_grad,
        output_grad,
        norm_grads[0],
        norm_grads[1],
        expand_grad,
        shrink_grad,
        norm_grads[2],
        norm_grads[3],
    )


def solution(mesh):
    tokens_spec = P(("dp", "mp"), None)
    vector = P(("dp", "mp"))
    in_specs = (
        tokens_spec,
        P("dp", "mp"),
        P("dp", "mp"),
        P("dp", "mp"),
        P("mp", None),
        P(None, ("dp", "mp")),
        vector,
        vector,
        P("dp", "mp"),
        P("mp", "dp"),
        vector,
        vector,
        P(),
        tokens_spec,
    )
    out_specs = (
        tokens_spec,
        tokens_spec,
        P("dp", "mp"),
        P("dp", "mp"),
        P("dp", "mp"),
        P("mp", None),
        P(None, ("dp", "mp")),
        vector,
        vector,
        P("dp", "mp"),
        P("mp", "dp"),
        vector,
        vector,
    )
    return jax.shard_map(
        on_device, mesh=mesh, in_specs=in_specs, out_specs=out_specs, check_vma=False
    )
```

```python
import functools
import jax
import jax.numpy as jnp
from jax import lax
from jax.experimental import pallas as pl
from jax.experimental.pallas import tpu as pltpu
from jax.sharding import PartitionSpec as P

HEAD_DIM = 64
LANDMARKS = 64
KERNEL = 33
PINV_STEPS = 6
HIGH = lax.Precision.HIGHEST
SCALE = HEAD_DIM ** (-0.5)
BLOCK = 256
MARGIN = 128
BF = jnp.bfloat16
F32 = jnp.float32


def nn(left, right, precision=None):
    return lax.dot_general(left, right, (((1,), (0,)), ((), ())), precision=precision, preferred_element_type=F32)


def nt(left, right, precision=None):
    return lax.dot_general(left, right, (((1,), (1,)), ((), ())), precision=precision, preferred_element_type=F32)


def tn(left, right, precision=None):
    return lax.dot_general(left, right, (((0,), (0,)), ((), ())), precision=precision, preferred_element_type=F32)


def split(values):
    high = values.astype(BF)
    return high, (values - high.astype(F32)).astype(BF)


def exact_left(left, right):
    high, rest = split(left)
    return nn(jnp.concatenate([high, rest], axis=1), jnp.concatenate([right, right], axis=0))


def exact_both(left, right):
    high, rest = split(left)
    right_high, right_rest = split(right)
    return nn(
        jnp.concatenate([high, rest, high], axis=1),
        jnp.concatenate([right_high, right_high, right_rest], axis=0),
    )


def exact_rows(left, right):
    high, rest = split(left)
    both = nt(jnp.concatenate([high, rest], axis=0), right)
    return both[: left.shape[0]] + both[left.shape[0] :]


def band(row):
    spread = jnp.broadcast_to(row, (2 * BLOCK, 2 * BLOCK))
    return pltpu.roll(spread, 0, 1, stride=1, stride_axis=0)[:, :BLOCK]


def convolve(values, row, padded):
    slots = values.shape[1]
    padded[...] = jnp.zeros(padded.shape, BF)
    padded[:, MARGIN : MARGIN + slots] = values
    windows = jnp.concatenate(
        [padded[:, b * BLOCK : (b + 2) * BLOCK] for b in range(slots // BLOCK)], axis=0
    )
    high, rest = split(band(row))
    result = nn(windows, high) + nn(windows, rest)
    d = values.shape[0]
    return jnp.concatenate(
        [result[b * d : (b + 1) * d] for b in range(slots // BLOCK)], axis=1
    )


def marks_kernel(q_ref, k_ref, member_t_ref, share_ref, mq_ref, mk_ref, a_ref, at_ref, z_ref):
    mq = nn(q_ref[...], member_t_ref[...]) * share_ref[...]
    mk = nn(k_ref[...], member_t_ref[...]) * share_ref[...]
    mq_ref[...] = mq
    mk_ref[...] = mk
    firsts, seconds, starts = [], [], []
    for h in range(2):
        part = slice(h * HEAD_DIM, (h + 1) * HEAD_DIM)
        scores = tn(mk[part], mq[part], HIGH) * SCALE
        grown = jnp.exp(scores - jnp.max(scores, axis=0, keepdims=True))
        second_t = grown / jnp.sum(grown, axis=0, keepdims=True)
        second = second_t.T
        widest = jnp.max(jnp.sum(second, axis=0, keepdims=True), axis=1, keepdims=True)
        firsts.append(second)
        seconds.append(second_t)
        starts.append(second_t / widest)
    a_ref[...] = jnp.concatenate(firsts, axis=1)
    at_ref[...] = jnp.concatenate(seconds, axis=1)
    z_ref[...] = jnp.concatenate(starts, axis=1)


def diagonal(values, mask):
    return jnp.where(mask, jnp.concatenate([values] * 4, axis=0), jnp.zeros((), BF))


def group_product(left, right, mask):
    high, rest = split(left)
    right_high, right_rest = split(right)
    both = nn(jnp.concatenate([high, rest], axis=0), diagonal(right_high, mask))
    return both[:LANDMARKS] + both[LANDMARKS:] + nn(high, diagonal(right_rest, mask))


def group_mask():
    width = 4 * LANDMARKS
    return (
        lax.broadcasted_iota(jnp.int32, (width, width), 0) // LANDMARKS
        == lax.broadcasted_iota(jnp.int32, (width, width), 1) // LANDMARKS
    )


def group_identity():
    shape = (LANDMARKS, 4 * LANDMARKS)
    return (
        lax.broadcasted_iota(jnp.int32, shape, 0)
        == lax.broadcasted_iota(jnp.int32, shape, 1) % LANDMARKS
    ).astype(F32)


def inverse_kernel(groups, a_ref, z0_ref, z_ref, kept_ref):
    mask, identity = group_mask(), group_identity()
    wide = 4 * LANDMARKS
    spans = [slice(g * wide, (g + 1) * wide) for g in range(groups)]
    a = [a_ref[:, s] for s in spans]
    z = [z0_ref[:, s] for s in spans]
    for step in range(PINV_STEPS):
        p = [group_product(x, y, mask) for x, y in zip(a, z)]
        t = [15.0 * identity - group_product(x, 7.0 * identity - x, mask) for x in p]
        u = [13.0 * identity - group_product(x, y, mask) for x, y in zip(p, t)]
        for s, zz, pp, tt, uu in zip(spans, z, p, t, u):
            kept_ref[step, 0, :, s] = zz
            kept_ref[step, 1, :, s] = pp
            kept_ref[step, 2, :, s] = tt
            kept_ref[step, 3, :, s] = uu
        z = [0.25 * group_product(x, y, mask) for x, y in zip(z, u)]
    for s, zz in zip(spans, z):
        z_ref[:, s] = zz


def inverse_back_kernel(groups, a_ref, at_ref, kept_ref, gz_ref, ds_ref):
    mask, identity = group_mask(), group_identity()
    wide = 4 * LANDMARKS
    spans = [slice(g * wide, (g + 1) * wide) for g in range(groups)]
    a = [a_ref[:, s] for s in spans]
    gz = [gz_ref[:, s] for s in spans]
    ga = [jnp.zeros_like(x) for x in a]
    for step in range(PINV_STEPS)[::-1]:
        z, p, t, u = ([kept_ref[step, i, :, s] for s in spans] for i in range(4))
        gu = [0.25 * group_product(x, y, mask) for x, y in zip(gz, z)]
        gt = [-group_product(x, y, mask) for x, y in zip(gu, p)]
        g7 = [-group_product(x, y, mask) for x, y in zip(gt, p)]
        gp = [
            -group_product(tt, guu, mask) - group_product(7.0 * identity - pp, gtt, mask) - gg
            for tt, guu, pp, gtt, gg in zip(t, gu, p, gt, g7)
        ]
        ga = [x + group_product(zz, g, mask) for x, zz, g in zip(ga, z, gp)]
        gz = [
            0.25 * group_product(uu, g, mask) + group_product(gpp, aa, mask)
            for uu, g, gpp, aa in zip(u, gz, gp, a)
        ]
    for s, aa, gaa, gzz in zip(spans, a, ga, gz):
        second_t = at_ref[:, s]
        sums = jnp.sum(aa, axis=0, keepdims=True)
        pieces = []
        for h in range(4):
            part = slice(h * LANDMARKS, (h + 1) * LANDMARKS)
            start_grad = gzz[:, part].T
            column = sums[:, part]
            widest = jnp.max(column, axis=1, keepdims=True)
            chosen = (column == widest).astype(F32)
            chosen = chosen / jnp.sum(chosen, axis=1, keepdims=True)
            at_h = second_t[:, part]
            widest_grad = -jnp.sum(
                jnp.sum(start_grad * at_h, axis=0, keepdims=True), axis=1, keepdims=True
            ) / (widest * widest)
            grad = gaa[:, part] + start_grad / widest
            grad = grad + jnp.transpose(
                jnp.broadcast_to(chosen * widest_grad, (LANDMARKS, LANDMARKS))
            )
            pieces.append((grad, at_h))
        for h, (grad, at_h) in enumerate(pieces):
            inner = jnp.sum(grad * at_h, axis=0, keepdims=True)
            pieces[h] = at_h * (grad - inner) * SCALE
        ds_ref[:, s] = jnp.concatenate(pieces, axis=1)


def forward_kernel(
    q_ref, k_ref, v_ref, mq_ref, mk_ref, z_ref, valid_ref, row_ref,
    out_ref, first_ref, third_ref, summary_ref, carried_ref, padded,
):
    valid = valid_ref[...]
    for h in range(2):
        part = slice(h * HEAD_DIM, (h + 1) * HEAD_DIM)
        q, k, v = q_ref[part, :], k_ref[part, :], v_ref[part, :]
        scores = exact_left(mk_ref[part, :].T, q) * SCALE
        grown = jnp.exp(scores - jnp.max(scores, axis=0, keepdims=True))
        first = grown / jnp.sum(grown, axis=0, keepdims=True)
        first_ref[part, :] = first
        scores = exact_left(mq_ref[part, :].T, k) * SCALE
        scores = jnp.where(valid > 0.0, scores, -1e30)
        grown = jnp.exp(scores - jnp.max(scores, axis=1, keepdims=True))
        third = grown / jnp.sum(grown, axis=1, keepdims=True)
        third_ref[part, :] = third
        summary = exact_rows(third, v)
        summary_ref[part, :] = summary
        carried = nn(z_ref[:, part], summary, HIGH)
        carried_ref[part, :] = carried
        mixed = exact_both(carried.T, first)
        masked = v * valid.astype(BF)
        mixed = mixed + convolve(masked, row_ref[h], padded)
        out_ref[part, :] = (mixed * valid).astype(BF)


def carried_back_kernel(d_ref, first_ref, z_ref, summary_ref, valid_ref, gz_ref, dsum_ref):
    valid = valid_ref[...].astype(BF)
    pieces = []
    for h in range(2):
        part = slice(h * HEAD_DIM, (h + 1) * HEAD_DIM)
        d_mixed = d_ref[part, :] * valid
        d_carried = exact_rows(first_ref[part, :], d_mixed)
        dsum_ref[part, :] = nn(z_ref[:, part].T, d_carried, HIGH)
        pieces.append(nt(summary_ref[part, :], d_carried, HIGH))
    gz_ref[...] = jnp.concatenate(pieces, axis=1)


def backward_kernel(
    d_ref, q_ref, k_ref, v_ref, first_ref, third_ref, mq_ref, mk_ref, carried_ref, dsum_ref,
    ds_ref, member_ref, share_ref, valid_ref, row_ref, dq_ref, dk_ref, dv_ref, taps_ref, padded,
):
    valid = valid_ref[...]
    low_valid = valid.astype(BF)
    member = member_ref[...]
    share = share_ref[...]
    slots = valid.shape[1]
    places = (MARGIN, MARGIN)
    turn = (
        lax.broadcasted_iota(jnp.int32, places, 0) + lax.broadcasted_iota(jnp.int32, places, 1)
        == MARGIN - 1
    ).astype(F32).astype(BF)
    for h in range(2):
        part = slice(h * HEAD_DIM, (h + 1) * HEAD_DIM)
        q, k, v = q_ref[part, :], k_ref[part, :], v_ref[part, :]
        d_mixed = d_ref[part, :] * low_valid
        mq_t, mk_t = mq_ref[part, :], mk_ref[part, :]
        first, third = first_ref[part, :], third_ref[part, :]
        d_first = exact_left(carried_ref[part, :], d_mixed)
        d_scores = first * (d_first - jnp.sum(first * d_first, axis=0, keepdims=True)) * SCALE
        d_query = exact_both(mk_t, d_scores)
        d_mk = exact_rows(d_scores, q).T
        d_summary = dsum_ref[part, :]
        d_third = exact_left(d_summary, v)
        d_scores = third * (d_third - jnp.sum(third * d_third, axis=1, keepdims=True)) * SCALE
        d_values = exact_both(d_summary.T, third)
        d_keys = exact_both(mq_t, d_scores)
        d_mq = exact_rows(d_scores, k).T
        ds_t = ds_ref[:, part]
        d_mq = (d_mq + nn(mk_t, ds_t, HIGH)) * share
        d_mk = (d_mk + nt(mq_t, ds_t, HIGH)) * share
        dq_ref[part, :] = (d_query + exact_left(d_mq, member)).astype(BF)
        dk_ref[part, :] = (d_keys + exact_left(d_mk, member)).astype(BF)
        d_values = d_values + convolve(d_mixed, row_ref[h], padded) * valid
        dv_ref[part, :] = d_values.astype(BF)
        masked = v * low_valid
        padded[:, MARGIN : MARGIN + slots] = masked
        step = 128
        total = tn(
            jnp.concatenate([d_mixed[:, b * step : (b + 1) * step] for b in range(slots // step)], axis=0),
            jnp.concatenate([padded[:, b * step : (b + 3) * step] for b in range(slots // step)], axis=0),
        )
        high, rest = split(total)
        turned = pltpu.roll(nn(turn, high) + nn(turn, rest), 0, 1, stride=1, stride_axis=0)
        taps_ref[h] = jnp.sum(turned, axis=0, keepdims=True)


def attention_setup(length, slots):
    positions = jnp.arange(slots, dtype=jnp.int32)
    valid = positions < length
    segment = positions * LANDMARKS // length
    marks = jnp.arange(LANDMARKS, dtype=jnp.int32)
    member = (segment[None, :] == marks[:, None]) & valid[None, :]
    member_t = (segment[:, None] == marks[None, :]) & valid[:, None]
    count = jnp.sum(member_t.astype(F32), axis=0, keepdims=True)
    return member.astype(BF), member_t.astype(BF), 1.0 / count, valid.astype(F32)[None, :]


def tap_rows(taps, reverse):
    taps = taps if reverse else taps[:, ::-1]
    start = 2 * BLOCK - MARGIN - KERNEL // 2
    rows = jnp.pad(taps, ((0, 0), (start, 2 * BLOCK - start - KERNEL)))
    return rows[:, None, :]


def specs(slots):
    big = pl.BlockSpec((2 * HEAD_DIM, slots), lambda i: (i, 0))
    thin = pl.BlockSpec((2 * HEAD_DIM, LANDMARKS), lambda i: (i, 0))
    side = pl.BlockSpec((LANDMARKS, 2 * LANDMARKS), lambda i: (0, i))
    return big, thin, side


def fixed(shape):
    return pl.BlockSpec(shape, lambda i: (0,) * len(shape))


def call(kernel, grid, in_specs, out_specs, out_shape, name, scratch=(), cost=None):
    return pl.pallas_call(
        kernel,
        grid=grid,
        in_specs=in_specs,
        out_specs=out_specs,
        out_shape=out_shape,
        scratch_shapes=list(scratch),
        name=name,
        compiler_params=pltpu.CompilerParams(vmem_limit_bytes=60 * 1024 * 1024),
        cost_estimate=cost,
    )


def shape(dims, kind=F32):
    return jax.ShapeDtypeStruct(dims, kind)


def cost_of(flops, moved):
    return pl.CostEstimate(flops=int(flops), bytes_accessed=int(moved), transcendentals=0)


def attention_forward(q, k, v, taps, setup):
    width, slots = q.shape
    pairs = width // (2 * HEAD_DIM)
    groups = width // (4 * HEAD_DIM)
    member, member_t, share, valid = setup
    big, thin, side = specs(slots)
    tall, flat = (width, LANDMARKS), (LANDMARKS, width)
    mq, mk, a, at, z0 = call(
        marks_kernel, (pairs,), [big, big, fixed(member_t.shape), fixed(share.shape)],
        [thin, thin, side, side, side], [shape(tall)] * 2 + [shape(flat)] * 3, "marks",
        cost=cost_of(2e9, 4e6),
    )(q, k, member_t, share)
    z, kept = call(
        functools.partial(inverse_kernel, groups), (1,), [fixed(flat), fixed(flat)],
        [fixed(flat), fixed((PINV_STEPS, 4) + flat)],
        [shape(flat), shape((PINV_STEPS, 4) + flat)], "inverse", cost=cost_of(8e9, 6e6),
    )(a, z0)
    row = pl.BlockSpec((2, 1, 2 * BLOCK), lambda i: (i, 0, 0))
    out, first, third, summary, carried = call(
        forward_kernel, (pairs,), [big, big, big, thin, thin, side, fixed(valid.shape), row],
        [big, big, big, thin, thin],
        [shape(q.shape, BF), shape(q.shape), shape(q.shape), shape(tall), shape(tall)],
        "forward", [pltpu.VMEM((HEAD_DIM, slots + MARGIN + BLOCK), BF)], cost=cost_of(1e10, 1.2e7),
    )(q, k, v, mq, mk, z, valid, tap_rows(taps, False))
    return out, (mq, mk, a, at, z, kept, first, third, summary, carried)


def attention_backward(d, q, k, v, taps, setup, saved):
    mq, mk, a, at, z, kept, first, third, summary, carried = saved
    width, slots = q.shape
    pairs = width // (2 * HEAD_DIM)
    groups = width // (4 * HEAD_DIM)
    member, member_t, share, valid = setup
    big, thin, side = specs(slots)
    tall, flat = (width, LANDMARKS), (LANDMARKS, width)
    gz, dsum = call(
        carried_back_kernel, (pairs,), [big, big, side, thin, fixed(valid.shape)], [side, thin],
        [shape(flat), shape(tall)], "carried_back", cost=cost_of(2e9, 5e6),
    )(d, first, z, summary, valid)
    ds = call(
        functools.partial(inverse_back_kernel, groups), (1,),
        [fixed(flat), fixed(flat), fixed((PINV_STEPS, 4) + flat), fixed(flat)], fixed(flat), shape(flat),
        "inverse_back", cost=cost_of(1.6e10, 6e6),
    )(a, at, kept, gz)
    row = pl.BlockSpec((2, 1, 2 * BLOCK), lambda i: (i, 0, 0))
    lags = pl.BlockSpec((2, 1, 384), lambda i: (i, 0, 0))
    dq, dk, dv, spread = call(
        backward_kernel, (pairs,),
        [big, big, big, big, big, big, thin, thin, thin, thin, side, fixed(member.shape),
         fixed(share.shape), fixed(valid.shape), row],
        [big, big, big, lags],
        [shape(q.shape, BF)] * 3 + [shape((2 * pairs, 1, 384))], "backward",
        [pltpu.VMEM((HEAD_DIM, slots + MARGIN + BLOCK), BF)], cost=cost_of(2e10, 1.6e7),
    )(d, q, k, v, first, third, mq, mk, carried, dsum, ds, member, share, valid, tap_rows(taps, True))
    start = 2 * MARGIN - 1 - KERNEL // 2
    return dq, dk, dv, spread[:, 0, start : start + KERNEL]


def ahead(left, right):
    return jnp.dot(left, right, preferred_element_type=jnp.float32)


def against(left, right):
    return lax.dot_general(
        left, right, (((1,), (1,)), ((), ())), preferred_element_type=jnp.float32
    )


def across(left, right):
    return lax.dot_general(
        left, right, (((0,), (0,)), ((), ())), preferred_element_type=jnp.float32
    )


def crossed(left, right):
    return lax.dot_general(
        left, right, (((0,), (1,)), ((), ())), preferred_element_type=jnp.float32
    )


def low(values):
    return values.astype(jnp.bfloat16)


def wide(values):
    return values.astype(jnp.float32)


def layer_norm(values, gain, bias):
    middle = jnp.mean(values, axis=-1, keepdims=True)
    centered = values - middle
    variance = jnp.mean(centered * centered, axis=-1, keepdims=True)
    return centered * lax.rsqrt(variance + 1e-05) * gain + bias


def exact_gelu(values):
    return jax.nn.gelu(values, approximate=False)


def bits_of(size):
    return max(size - 1, 0).bit_length()


def flip(values, bit):
    size = lax.axis_size("dp")
    return lax.ppermute(values, "dp", [(i, i ^ (1 << bit)) for i in range(size)])


def partner(values):
    size = lax.axis_size("mp")
    return lax.ppermute(values, "mp", [(i, (i + 1) % size) for i in range(size)])


def spread_small(values):
    group = lax.axis_index("dp")
    values = values[:, None, :]
    for bit in range(bits_of(lax.axis_size("dp"))):
        other = flip(values, bit)
        upper = ((group >> bit) & 1) == 1
        values = jnp.where(
            upper,
            jnp.concatenate([other, values], axis=1),
            jnp.concatenate([values, other], axis=1),
        )
    return values.reshape(values.shape[0], -1)


def sum_all(values):
    for bit in range(bits_of(lax.axis_size("dp"))):
        values = values + flip(values, bit)
    return values


def fold(blocks, orders, kind):
    count = bits_of(lax.axis_size("dp"))
    group = lax.axis_index("dp")
    columns = blocks.shape[2]
    edges = [round(columns / 128 * i / len(orders)) * 128 for i in range(len(orders))] + [columns]
    pieces = []
    for color, order in enumerate(orders):
        if edges[color] == edges[color + 1]:
            continue
        part = blocks[:, :, edges[color] : edges[color + 1]]
        part = part.reshape((2,) * count + part.shape[1:])
        left = list(range(count))[::-1]
        for place, bit in enumerate(order):
            axis = left.index(bit)
            mine = (group >> bit) & 1
            keep = lax.dynamic_index_in_dim(part, mine, axis, keepdims=False)
            send = lax.dynamic_index_in_dim(part, 1 - mine, axis, keepdims=False)
            part = wide(keep) + wide(flip(send.astype(kind), bit))
            if place + 1 < count:
                part = part.astype(kind)
            left.pop(axis)
        pieces.append(part)
    return jnp.concatenate(pieces, axis=1) if len(pieces) > 1 else pieces[0]


def color_orders():
    count = bits_of(lax.axis_size("dp"))
    base = list(range(count))
    return [base, base[1:] + base[:1], base[2:] + base[:2]]


def on_device(
    tokens,
    w_query,
    w_key,
    w_value,
    value_taps,
    w_output,
    first_gain,
    first_bias,
    w_expand,
    w_shrink,
    second_gain,
    second_bias,
    doc_lengths,
    out_grad,
):
    parts = lax.axis_size("mp")
    groups = lax.axis_size("dp")
    group = lax.axis_index("dp")
    core = lax.axis_index("mp")
    slots, width = tokens.shape
    half = w_query.shape[1]
    hidden_half = w_expand.shape[1]
    rows = w_query.shape[0]
    length = lax.dynamic_index_in_dim(doc_lengths, group * parts + core, 0, keepdims=False)

    def in_core_order(own, other, axis):
        return jnp.where(
            core == 0,
            jnp.concatenate([own, other], axis=axis),
            jnp.concatenate([other, own], axis=axis),
        )

    output_t = w_output.T
    mine_cols = lax.dynamic_slice_in_dim(output_t, core * half, half, 1)
    their_cols = lax.dynamic_slice_in_dim(output_t, (1 - core) * half, half, 1)
    output_block = in_core_order(mine_cols, partner(their_cols), 0)
    head_block = jnp.concatenate([w_query, w_key, w_value, output_block], axis=1)
    hidden_block = jnp.concatenate([w_expand, w_shrink.T], axis=1)
    head_own = lax.all_gather(head_block, "dp", axis=0, tiled=True)
    head_other = partner(head_own)
    hidden_own = lax.all_gather(hidden_block, "dp", axis=0, tiled=True)
    hidden_other = partner(hidden_own)
    norms = jnp.stack([first_gain, first_bias, second_gain, second_bias])
    norms = in_core_order(norms, partner(norms), 1)
    gain_one, bias_one, gain_two, bias_two = wide(spread_small(norms))
    taps = jnp.concatenate([value_taps, partner(value_taps)], axis=0)

    def part_of(block, index, size):
        return block[:, index * size : (index + 1) * size]

    def both(index):
        return part_of(head_own, index, half), part_of(head_other, index, half)

    q_own, q_oth = both(0)
    k_own, k_oth = both(1)
    v_own, v_oth = both(2)
    o_own, o_oth = both(3)
    e_own, s_own = part_of(hidden_own, 0, hidden_half), part_of(hidden_own, 1, hidden_half)
    e_oth, s_oth = part_of(hidden_other, 0, hidden_half), part_of(hidden_other, 1, hidden_half)

    def project(own, oth):
        return jnp.concatenate([low(crossed(own, tokens)), low(crossed(oth, tokens))], axis=0)

    query, keys, values = project(q_own, q_oth), project(k_own, k_oth), project(v_own, v_oth)
    setup = attention_setup(length, slots)
    attended, saved = attention_forward(query, keys, values, taps, setup)
    att_own, att_oth = attended[:half], attended[half:]
    projected = crossed(att_own, o_own) + crossed(att_oth, o_oth)
    first_out, first_back = jax.vjp(layer_norm, wide(tokens) + projected, gain_one, bias_one)
    hidden_in = low(first_out)
    act_own, gelu_own = jax.vjp(exact_gelu, ahead(hidden_in, e_own))
    act_oth, gelu_oth = jax.vjp(exact_gelu, ahead(hidden_in, e_oth))
    act_own, act_oth = low(act_own), low(act_oth)
    branch = against(act_own, s_own) + against(act_oth, s_oth)
    result, second_back = jax.vjp(layer_norm, first_out + branch, gain_two, bias_two)
    layer_out = low(result)
    d_second_in, gain_two_grad, bias_two_grad = second_back(wide(out_grad))
    d_branch = low(d_second_in)
    (d_pre_oth,) = gelu_oth(ahead(d_branch, s_oth))
    d_pre_oth = low(d_pre_oth)
    shrink_send = low(across(d_branch, act_oth))
    expand_send = low(across(hidden_in, d_pre_oth))
    shrink_got, expand_got = partner(shrink_send), partner(expand_send)
    (d_pre_own,) = gelu_own(ahead(d_branch, s_own))
    d_pre_own = low(d_pre_own)
    shrink_sum = low(across(d_branch, act_own) + wide(shrink_got))
    expand_sum = low(across(hidden_in, d_pre_own) + wide(expand_got))
    orders = color_orders()

    def blocks(values):
        return values.reshape(groups, rows, values.shape[1])

    shrink_grad = fold(blocks(shrink_sum), orders, jnp.bfloat16).T
    expand_grad = fold(blocks(expand_sum), orders, jnp.bfloat16)
    d_hidden = against(d_pre_own, e_own) + against(d_pre_oth, e_oth)
    d_first_in, gain_one_grad, bias_one_grad = first_back(d_second_in + d_hidden)
    d_projected = low(d_first_in)
    d_attended = jnp.concatenate(
        [low(crossed(o_own, d_projected)), low(crossed(o_oth, d_projected))], axis=0
    )
    norm_grads = jnp.stack([gain_one_grad, bias_one_grad, gain_two_grad, bias_two_grad])
    norm_grads = norm_grads + partner(norm_grads)
    norm_grads = fold(
        norm_grads.reshape(4, groups, rows).swapaxes(0, 1), orders[:1], jnp.float32
    )
    norm_grads = lax.dynamic_slice_in_dim(norm_grads, core * (rows // parts), rows // parts, 1)
    d_query, d_keys, d_values, taps_grad = attention_backward(
        d_attended, query, keys, values, taps, setup, saved
    )
    taps_grad = sum_all(taps_grad[: taps_grad.shape[0] // 2] + partner(taps_grad[taps_grad.shape[0] // 2 :]))

    def owned(values):
        return values[:half]

    def others(values):
        return values[half:]

    head_send = low(
        jnp.concatenate(
            [
                crossed(tokens, others(d_query)),
                crossed(tokens, others(d_keys)),
                crossed(tokens, others(d_values)),
                crossed(d_projected, att_oth),
            ],
            axis=1,
        )
    )
    head_got = partner(head_send)
    head_sum = low(
        jnp.concatenate(
            [
                crossed(tokens, owned(d_query)),
                crossed(tokens, owned(d_keys)),
                crossed(tokens, owned(d_values)),
                crossed(d_projected, att_own),
            ],
            axis=1,
        )
        + wide(head_got)
    )
    head_grads = fold(blocks(head_sum), orders, jnp.bfloat16)
    tokens_grad = d_first_in + (
        crossed(owned(d_query), q_own)
        + crossed(others(d_query), q_oth)
        + crossed(owned(d_keys), k_own)
        + crossed(others(d_keys), k_oth)
        + crossed(owned(d_values), v_own)
        + crossed(others(d_values), v_oth)
    )
    query_grad, key_grad, value_grad, output_part = (
        head_grads[:, i * half : (i + 1) * half] for i in range(4)
    )
    keep_rows = lax.dynamic_slice_in_dim(output_part, core * (rows // parts), rows // parts, 0)
    send_rows = lax.dynamic_slice_in_dim(output_part, (1 - core) * (rows // parts), rows // parts, 0)
    output_grad = in_core_order(keep_rows, partner(send_rows), 1).T
    return (
        layer_out,
        tokens_grad,
        query_grad,
        key_grad,
        value_grad,
        taps_grad,
        output_grad,
        norm_grads[0],
        norm_grads[1],
        expand_grad,
        shrink_grad,
        norm_grads[2],
        norm_grads[3],
    )


def solution(mesh):
    tokens_spec = P(("dp", "mp"), None)
    vector = P(("dp", "mp"))
    in_specs = (
        tokens_spec,
        P("dp", "mp"),
        P("dp", "mp"),
        P("dp", "mp"),
        P("mp", None),
        P(None, ("dp", "mp")),
        vector,
        vector,
        P("dp", "mp"),
        P("mp", "dp"),
        vector,
        vector,
        P(),
        tokens_spec,
    )
    out_specs = (
        tokens_spec,
        tokens_spec,
        P("dp", "mp"),
        P("dp", "mp"),
        P("dp", "mp"),
        P("mp", None),
        P(None, ("dp", "mp")),
        vector,
        vector,
        P("dp", "mp"),
        P("mp", "dp"),
        vector,
        vector,
    )
    return jax.shard_map(
        on_device, mesh=mesh, in_specs=in_specs, out_specs=out_specs, check_vma=False
    )
```

```python
import functools
import jax
import jax.numpy as jnp
from jax import lax
from jax.experimental import pallas as pl
from jax.experimental.pallas import tpu as pltpu
from jax.sharding import PartitionSpec as P

HEAD_DIM = 64
LANDMARKS = 64
KERNEL = 33
PINV_STEPS = 6
HIGH = lax.Precision.HIGHEST
SCALE = HEAD_DIM ** (-0.5)
BLOCK = 256
MARGIN = 128
WHEN = (0, 7, 10, 12)
GATHER_WHEN = (5, 11)
TILE = 512
CHUNK = 256
BF = jnp.bfloat16
F32 = jnp.float32


def nn(left, right, precision=None):
    return lax.dot_general(left, right, (((1,), (0,)), ((), ())), precision=precision, preferred_element_type=F32)


def nt(left, right, precision=None):
    return lax.dot_general(left, right, (((1,), (1,)), ((), ())), precision=precision, preferred_element_type=F32)


def tn(left, right, precision=None):
    return lax.dot_general(left, right, (((0,), (0,)), ((), ())), precision=precision, preferred_element_type=F32)


def split(values):
    high = values.astype(BF)
    return high, (values - high.astype(F32)).astype(BF)


def exact_left(left, right):
    high, rest = split(left)
    return nn(jnp.concatenate([high, rest], axis=1), jnp.concatenate([right, right], axis=0))


def exact_both(left, right):
    high, rest = split(left)
    right_high, right_rest = split(right)
    return nn(
        jnp.concatenate([high, rest, high], axis=1),
        jnp.concatenate([right_high, right_high, right_rest], axis=0),
    )


def exact_rows(left, right):
    high, rest = split(left)
    both = nt(jnp.concatenate([high, rest], axis=0), right)
    return both[: left.shape[0]] + both[left.shape[0] :]


def band(row):
    spread = jnp.broadcast_to(row, (2 * BLOCK, 2 * BLOCK))
    return pltpu.roll(spread, 0, 1, stride=1, stride_axis=0)[:, :BLOCK]


def convolve(values, row, padded):
    slots = values.shape[1]
    padded[...] = jnp.zeros(padded.shape, BF)
    padded[:, MARGIN : MARGIN + slots] = values
    windows = jnp.concatenate(
        [padded[:, b * BLOCK : (b + 2) * BLOCK] for b in range(slots // BLOCK)], axis=0
    )
    high, rest = split(band(row))
    result = nn(windows, high) + nn(windows, rest)
    d = values.shape[0]
    return jnp.concatenate(
        [result[b * d : (b + 1) * d] for b in range(slots // BLOCK)], axis=1
    )


def marks_kernel(q_ref, k_ref, member_t_ref, share_ref, mq_ref, mk_ref, a_ref, at_ref, z_ref):
    mq = nn(q_ref[...], member_t_ref[...]) * share_ref[...]
    mk = nn(k_ref[...], member_t_ref[...]) * share_ref[...]
    mq_ref[...] = mq
    mk_ref[...] = mk
    firsts, seconds, starts = [], [], []
    for h in range(2):
        part = slice(h * HEAD_DIM, (h + 1) * HEAD_DIM)
        scores = tn(mk[part], mq[part], HIGH) * SCALE
        grown = jnp.exp(scores - jnp.max(scores, axis=0, keepdims=True))
        second_t = grown / jnp.sum(grown, axis=0, keepdims=True)
        second = second_t.T
        widest = jnp.max(jnp.sum(second, axis=0, keepdims=True), axis=1, keepdims=True)
        firsts.append(second)
        seconds.append(second_t)
        starts.append(second_t / widest)
    a_ref[...] = jnp.concatenate(firsts, axis=1)
    at_ref[...] = jnp.concatenate(seconds, axis=1)
    z_ref[...] = jnp.concatenate(starts, axis=1)


def diagonal(values, mask):
    return jnp.where(mask, jnp.concatenate([values] * 4, axis=0), jnp.zeros((), BF))


def group_product(left, right, mask):
    high, rest = split(left)
    right_high, right_rest = split(right)
    both = nn(jnp.concatenate([high, rest], axis=0), diagonal(right_high, mask))
    return both[:LANDMARKS] + both[LANDMARKS:] + nn(high, diagonal(right_rest, mask))


def group_mask():
    width = 4 * LANDMARKS
    return (
        lax.broadcasted_iota(jnp.int32, (width, width), 0) // LANDMARKS
        == lax.broadcasted_iota(jnp.int32, (width, width), 1) // LANDMARKS
    )


def group_identity():
    shape = (LANDMARKS, 4 * LANDMARKS)
    return (
        lax.broadcasted_iota(jnp.int32, shape, 0)
        == lax.broadcasted_iota(jnp.int32, shape, 1) % LANDMARKS
    ).astype(F32)


def inverse_kernel(groups, a_ref, z0_ref, z_ref, kept_ref):
    mask, identity = group_mask(), group_identity()
    wide = 4 * LANDMARKS
    spans = [slice(g * wide, (g + 1) * wide) for g in range(groups)]
    a = [a_ref[:, s] for s in spans]
    z = [z0_ref[:, s] for s in spans]
    for step in range(PINV_STEPS):
        p = [group_product(x, y, mask) for x, y in zip(a, z)]
        t = [15.0 * identity - group_product(x, 7.0 * identity - x, mask) for x in p]
        u = [13.0 * identity - group_product(x, y, mask) for x, y in zip(p, t)]
        for s, zz, pp, tt, uu in zip(spans, z, p, t, u):
            kept_ref[step, 0, :, s] = zz
            kept_ref[step, 1, :, s] = pp
            kept_ref[step, 2, :, s] = tt
            kept_ref[step, 3, :, s] = uu
        z = [0.25 * group_product(x, y, mask) for x, y in zip(z, u)]
    for s, zz in zip(spans, z):
        z_ref[:, s] = zz


def inverse_back_kernel(groups, a_ref, at_ref, kept_ref, gz_ref, ds_ref):
    mask, identity = group_mask(), group_identity()
    wide = 4 * LANDMARKS
    spans = [slice(g * wide, (g + 1) * wide) for g in range(groups)]
    a = [a_ref[:, s] for s in spans]
    gz = [gz_ref[:, s] for s in spans]
    ga = [jnp.zeros_like(x) for x in a]
    for step in range(PINV_STEPS)[::-1]:
        z, p, t, u = ([kept_ref[step, i, :, s] for s in spans] for i in range(4))
        gu = [0.25 * group_product(x, y, mask) for x, y in zip(gz, z)]
        gt = [-group_product(x, y, mask) for x, y in zip(gu, p)]
        g7 = [-group_product(x, y, mask) for x, y in zip(gt, p)]
        gp = [
            -group_product(tt, guu, mask) - group_product(7.0 * identity - pp, gtt, mask) - gg
            for tt, guu, pp, gtt, gg in zip(t, gu, p, gt, g7)
        ]
        ga = [x + group_product(zz, g, mask) for x, zz, g in zip(ga, z, gp)]
        gz = [
            0.25 * group_product(uu, g, mask) + group_product(gpp, aa, mask)
            for uu, g, gpp, aa in zip(u, gz, gp, a)
        ]
    for s, aa, gaa, gzz in zip(spans, a, ga, gz):
        second_t = at_ref[:, s]
        sums = jnp.sum(aa, axis=0, keepdims=True)
        pieces = []
        for h in range(4):
            part = slice(h * LANDMARKS, (h + 1) * LANDMARKS)
            start_grad = gzz[:, part].T
            column = sums[:, part]
            widest = jnp.max(column, axis=1, keepdims=True)
            chosen = (column == widest).astype(F32)
            chosen = chosen / jnp.sum(chosen, axis=1, keepdims=True)
            at_h = second_t[:, part]
            widest_grad = -jnp.sum(
                jnp.sum(start_grad * at_h, axis=0, keepdims=True), axis=1, keepdims=True
            ) / (widest * widest)
            grad = gaa[:, part] + start_grad / widest
            grad = grad + jnp.transpose(
                jnp.broadcast_to(chosen * widest_grad, (LANDMARKS, LANDMARKS))
            )
            pieces.append((grad, at_h))
        for h, (grad, at_h) in enumerate(pieces):
            inner = jnp.sum(grad * at_h, axis=0, keepdims=True)
            pieces[h] = at_h * (grad - inner) * SCALE
        ds_ref[:, s] = jnp.concatenate(pieces, axis=1)


def forward_kernel(
    q_ref, k_ref, v_ref, mq_ref, mk_ref, z_ref, valid_ref, row_ref,
    out_ref, first_ref, third_ref, summary_ref, carried_ref, padded,
):
    valid = valid_ref[...]
    for h in range(2):
        part = slice(h * HEAD_DIM, (h + 1) * HEAD_DIM)
        q, k, v = q_ref[part, :], k_ref[part, :], v_ref[part, :]
        scores = exact_left(mk_ref[part, :].T, q) * SCALE
        grown = jnp.exp(scores - jnp.max(scores, axis=0, keepdims=True))
        first = grown / jnp.sum(grown, axis=0, keepdims=True)
        first_ref[part, :] = first
        scores = exact_left(mq_ref[part, :].T, k) * SCALE
        scores = jnp.where(valid > 0.0, scores, -1e30)
        grown = jnp.exp(scores - jnp.max(scores, axis=1, keepdims=True))
        third = grown / jnp.sum(grown, axis=1, keepdims=True)
        third_ref[part, :] = third
        summary = exact_rows(third, v)
        summary_ref[part, :] = summary
        carried = nn(z_ref[:, part], summary, HIGH)
        carried_ref[part, :] = carried
        mixed = exact_both(carried.T, first)
        masked = v * valid.astype(BF)
        mixed = mixed + convolve(masked, row_ref[h], padded)
        out_ref[part, :] = (mixed * valid).astype(BF)


def carried_back_kernel(d_ref, first_ref, z_ref, summary_ref, valid_ref, gz_ref, dsum_ref):
    valid = valid_ref[...].astype(BF)
    pieces = []
    for h in range(2):
        part = slice(h * HEAD_DIM, (h + 1) * HEAD_DIM)
        d_mixed = d_ref[part, :] * valid
        d_carried = exact_rows(first_ref[part, :], d_mixed)
        dsum_ref[part, :] = nn(z_ref[:, part].T, d_carried, HIGH)
        pieces.append(nt(summary_ref[part, :], d_carried, HIGH))
    gz_ref[...] = jnp.concatenate(pieces, axis=1)


def backward_kernel(
    d_ref, q_ref, k_ref, v_ref, first_ref, third_ref, mq_ref, mk_ref, carried_ref, dsum_ref,
    ds_ref, member_ref, share_ref, valid_ref, row_ref, dq_ref, dk_ref, dv_ref, taps_ref, padded,
):
    valid = valid_ref[...]
    low_valid = valid.astype(BF)
    member = member_ref[...]
    share = share_ref[...]
    slots = valid.shape[1]
    places = (MARGIN, MARGIN)
    turn = (
        lax.broadcasted_iota(jnp.int32, places, 0) + lax.broadcasted_iota(jnp.int32, places, 1)
        == MARGIN - 1
    ).astype(F32).astype(BF)
    for h in range(2):
        part = slice(h * HEAD_DIM, (h + 1) * HEAD_DIM)
        q, k, v = q_ref[part, :], k_ref[part, :], v_ref[part, :]
        d_mixed = d_ref[part, :] * low_valid
        mq_t, mk_t = mq_ref[part, :], mk_ref[part, :]
        first, third = first_ref[part, :], third_ref[part, :]
        d_first = exact_left(carried_ref[part, :], d_mixed)
        d_scores = first * (d_first - jnp.sum(first * d_first, axis=0, keepdims=True)) * SCALE
        d_query = exact_both(mk_t, d_scores)
        d_mk = exact_rows(d_scores, q).T
        d_summary = dsum_ref[part, :]
        d_third = exact_left(d_summary, v)
        d_scores = third * (d_third - jnp.sum(third * d_third, axis=1, keepdims=True)) * SCALE
        d_values = exact_both(d_summary.T, third)
        d_keys = exact_both(mq_t, d_scores)
        d_mq = exact_rows(d_scores, k).T
        ds_t = ds_ref[:, part]
        d_mq = (d_mq + nn(mk_t, ds_t, HIGH)) * share
        d_mk = (d_mk + nt(mq_t, ds_t, HIGH)) * share
        dq_ref[part, :] = (d_query + exact_left(d_mq, member)).astype(BF)
        dk_ref[part, :] = (d_keys + exact_left(d_mk, member)).astype(BF)
        d_values = d_values + convolve(d_mixed, row_ref[h], padded) * valid
        dv_ref[part, :] = d_values.astype(BF)
        masked = v * low_valid
        padded[:, MARGIN : MARGIN + slots] = masked
        step = 128
        total = tn(
            jnp.concatenate([d_mixed[:, b * step : (b + 1) * step] for b in range(slots // step)], axis=0),
            jnp.concatenate([padded[:, b * step : (b + 3) * step] for b in range(slots // step)], axis=0),
        )
        high, rest = split(total)
        turned = pltpu.roll(nn(turn, high) + nn(turn, rest), 0, 1, stride=1, stride_axis=0)
        taps_ref[h] = jnp.sum(turned, axis=0, keepdims=True)


def membership(length, slots, turned):
    dims = (slots, LANDMARKS) if turned else (LANDMARKS, slots)
    mark = lax.broadcasted_iota(jnp.int32, dims, 1 if turned else 0)
    position = lax.broadcasted_iota(jnp.int32, dims, 0 if turned else 1)
    low_end = position * LANDMARKS >= mark * length
    high_end = position * LANDMARKS < (mark + 1) * length
    inside = jnp.logical_and(jnp.logical_and(low_end, high_end), position < length)
    return inside.astype(F32)


def tap_rows(taps, reverse):
    taps = taps if reverse else taps[:, ::-1]
    start = 2 * BLOCK - MARGIN - KERNEL // 2
    rows = jnp.pad(taps, ((0, 0), (start, 2 * BLOCK - start - KERNEL)))
    return rows[:, None, :]


def specs(slots):
    big = pl.BlockSpec((2 * HEAD_DIM, slots), lambda i: (i, 0))
    thin = pl.BlockSpec((2 * HEAD_DIM, LANDMARKS), lambda i: (i, 0))
    side = pl.BlockSpec((LANDMARKS, 2 * LANDMARKS), lambda i: (0, i))
    return big, thin, side


def fixed(shape):
    return pl.BlockSpec(shape, lambda i: (0,) * len(shape))


def call(kernel, grid, in_specs, out_specs, out_shape, name, scratch=(), cost=None):
    return pl.pallas_call(
        kernel,
        grid=grid,
        in_specs=in_specs,
        out_specs=out_specs,
        out_shape=out_shape,
        scratch_shapes=list(scratch),
        name=name,
        compiler_params=pltpu.CompilerParams(vmem_limit_bytes=60 * 1024 * 1024),
        cost_estimate=cost,
    )


def shape(dims, kind=F32):
    return jax.ShapeDtypeStruct(dims, kind)


def cost_of(flops, moved):
    return pl.CostEstimate(flops=int(flops), bytes_accessed=int(moved), transcendentals=0)


def ahead(left, right):
    return jnp.dot(left, right, preferred_element_type=jnp.float32)


def against(left, right):
    return lax.dot_general(
        left, right, (((1,), (1,)), ((), ())), preferred_element_type=jnp.float32
    )


def across(left, right):
    return lax.dot_general(
        left, right, (((0,), (0,)), ((), ())), preferred_element_type=jnp.float32
    )


def crossed(left, right):
    return lax.dot_general(
        left, right, (((0,), (1,)), ((), ())), preferred_element_type=jnp.float32
    )


def low(values):
    return values.astype(jnp.bfloat16)


def wide(values):
    return values.astype(jnp.float32)


def layer_norm(values, gain, bias):
    middle = jnp.mean(values, axis=-1, keepdims=True)
    centered = values - middle
    variance = jnp.mean(centered * centered, axis=-1, keepdims=True)
    return centered * lax.rsqrt(variance + 1e-05) * gain + bias


def exact_gelu(values):
    return jax.nn.gelu(values, approximate=False)


def partner(values):
    size = lax.axis_size("mp")
    return lax.ppermute(values, "mp", [(i, (i + 1) % size) for i in range(size)])


def bits_of(size):
    return max(size - 1, 0).bit_length()


def scatter_orders(count):
    if count < 4:
        return [list(range(count))] * 6
    x, y, near, far = [0], [1], [2], list(range(3, count))
    return [
        far + y + x + near, y + far + x + near, x + y + far + near,
        near + x + y + far, x + near + y + far, y + x + near + far,
    ]


def colored(widths, orders):
    streams, turn = [], 0
    for piece, columns in enumerate(widths):
        tiles = columns // 128
        if tiles >= 12:
            chosen = orders
        elif tiles >= 3:
            chosen, turn = orders[3 * turn : 3 * turn + 3], 1 - turn
        else:
            chosen = orders[:1]
        cuts = [round(tiles * part / len(chosen)) * 128 for part in range(len(chosen))] + [columns]
        for low_edge, high_edge, order in zip(cuts[:-1], cuts[1:], chosen):
            if high_edge > low_edge:
                streams.append((piece, low_edge, high_edge, order))
    return streams


def neighbours(count):
    group = lax.axis_index("dp")
    mine = [(group // 2**b) % 2 for b in range(count)]
    return group, mine, [group + (1 - 2 * mine[b]) * 2**b for b in range(count)]


def enter(group, across_bits, core):
    barrier = pltpu.get_barrier_semaphore()
    for other in across_bits:
        pl.semaphore_signal(
            barrier, inc=1, device_id=(other, core), device_id_type=pl.DeviceIdType.MESH
        )
    pl.semaphore_signal(
        barrier, inc=1, device_id=(group, 1 - core), device_id_type=pl.DeviceIdType.MESH
    )
    pl.semaphore_wait(barrier, len(across_bits) + 1)


def remote(source, target, send, arrive, device):
    return pltpu.make_async_remote_copy(
        src_ref=source,
        dst_ref=target,
        send_sem=send,
        recv_sem=arrive,
        device_id=device,
        device_id_type=pl.DeviceIdType.MESH,
    )


def gather_kernel(count, streams, partial, whole, *refs):
    pieces = whole + len(partial)
    blocks, refs = refs[:pieces], refs[pieces:]
    owns, refs = refs[:whole], refs[whole:]
    others, refs = refs[:whole], refs[whole:]
    parts, refs = refs[: len(partial)], refs[len(partial) :]
    send, arrive, side_send, side_arrive, first_send, first_arrive, local = refs
    group, mine, across_bits = neighbours(count)
    core = lax.axis_index("mp")
    twin = (group, 1 - core)

    def view(ref, chosen, columns):
        place = tuple(chosen[b] for b in sorted(chosen, reverse=True))
        return ref.at[place + (slice(None), columns)]

    def own_view(index, chosen):
        piece, low_edge, high_edge, order = streams[index]
        columns = slice(low_edge, high_edge)
        if piece < whole:
            return view(owns[piece], chosen, columns)
        return view(parts[piece - whole], {b: chosen[b] for b in order}, columns)

    def hop(index, place):
        piece, low_edge, high_edge, order = streams[index]
        chosen = {b: slice(None) if b in order[:place] else mine[b] for b in range(count)}
        target = own_view(index, chosen)
        source = blocks[piece].at[:, slice(low_edge, high_edge)] if place == 0 else target
        return remote(
            source, target, send.at[index, place], arrive.at[index, place],
            (across_bits[order[place]], core),
        )

    def forward(index, place):
        piece, low_edge, high_edge, order = streams[index]
        chosen = {b: slice(None) if b in order[:place] else mine[b] for b in range(count)}
        chosen[order[place]] = 1 - mine[order[place]]
        columns = slice(low_edge, high_edge)
        return remote(
            view(owns[piece], chosen, columns), view(others[piece], chosen, columns),
            side_send.at[index, place], side_arrive.at[index, place], twin,
        )

    place_of = {b: mine[b] for b in range(count)}
    enter(group, across_bits, core)
    full = [index for index, stream in enumerate(streams) if stream[0] < whole]
    thin = [index for index, stream in enumerate(streams) if stream[0] >= whole]
    copies, sides = [], []
    hops = {}
    for index in full:
        hops[index] = hop(index, 0)
        hops[index].start()
    for p in range(whole):
        copy = pltpu.make_async_copy(
            blocks[p], view(owns[p], place_of, slice(None)), local.at[p]
        )
        copy.start()
        copies.append(copy)
        side = remote(
            blocks[p], view(others[p], place_of, slice(None)), first_send.at[p],
            first_arrive.at[p], twin,
        )
        side.start()
        sides.append(side)
    lasts = []
    for index in thin:
        piece, low_edge, high_edge, order = streams[index]
        copy = pltpu.make_async_copy(
            blocks[piece].at[:, slice(low_edge, high_edge)], own_view(index, place_of),
            local.at[whole + index - len(full)],
        )
        copy.start()
        lasts.append(copy)
    for copy in copies:
        copy.wait()
    sent = []

    def advance(index, place, places):
        hops[index].wait_recv()
        sent.append(hops[index])
        if place + 1 < places:
            hops[index] = hop(index, place + 1)
            hops[index].start()

    for place in range(count):
        for index in full:
            advance(index, place, count)
            side = forward(index, place)
            side.start()
            sides.append(side)
        if place == count - 3:
            for index in thin:
                hops[index] = hop(index, 0)
                hops[index].start()
            for copy in lasts:
                copy.wait()
        if place == count - 2:
            for step in range(count - 2):
                if step + 1 < count - 2:
                    for index in thin:
                        advance(index, step, count - 2)
    for index in thin:
        advance(index, count - 3, count - 2)
    for one in sent:
        one.wait_send()
    for side in sides:
        side.wait()


def gather_streams(blocks, count, first):
    orders = [order[::-1] for order in scatter_orders(count)]
    return [
        (piece + first, low_edge, high_edge, order)
        for piece, low_edge, high_edge, order in colored([b.shape[1] for b in blocks], orders)
    ]


def gather(blocks, partial, identity):
    groups = lax.axis_size("dp")
    count = bits_of(groups)
    streams = gather_streams(blocks, count, 0)
    full = len(streams)
    streams += [
        (piece, low_edge, high_edge, order[: count - 2])
        for piece, low_edge, high_edge, order in gather_streams(partial, count, len(blocks))
    ]
    results = [jax.ShapeDtypeStruct((2,) * count + b.shape, b.dtype) for b in blocks] * 2
    results += [jax.ShapeDtypeStruct((2,) * (count - 2) + b.shape, b.dtype) for b in partial]
    dma = pltpu.SemaphoreType.DMA
    anywhere = pl.BlockSpec(memory_space=pl.ANY)
    outs = pl.pallas_call(
        functools.partial(gather_kernel, count, streams, partial, len(blocks)),
        in_specs=[pl.BlockSpec(memory_space=pltpu.VMEM)] * (len(blocks) + len(partial)),
        out_specs=[anywhere] * len(results),
        out_shape=results,
        scratch_shapes=[dma((len(streams), count))] * 2
        + [dma((full, count))] * 2
        + [dma((len(blocks),))] * 2
        + [dma((len(blocks) + len(streams) - full,))],
        name="gather",
        compiler_params=pltpu.CompilerParams(collective_id=identity, has_side_effects=True),
    )(*blocks, *partial)
    whole = len(blocks)
    flat = [o.reshape((groups,) + o.shape[count:]) for o in outs[: 2 * whole]]
    return list(zip(flat[:whole], flat[whole:])), outs[2 * whole :]


def lead_kernel(count, streams, groups, pieces, *refs):
    (tokens_ref, lengths_ref, row_ref), refs = refs[:3], refs[3:]
    own_weights, other_weights, refs = refs[:3], refs[3:6], refs[6:]
    parts, refs = refs[:pieces], refs[pieces:]
    (
        q_ref, k_ref, v_ref, out_ref, first_ref, third_ref, summary_ref, carried_ref, mq_ref, mk_ref, a_ref, at_ref,
        z_ref, kept_ref, tokens_t_ref, member_ref, share_ref, valid_ref,
    ), refs = refs[:18], refs[18:]
    owns, refs = refs[:pieces], refs[pieces:]
    others, refs = refs[:pieces], refs[pieces:]
    held, refs = refs[:pieces], refs[pieces:]
    start_ref, padded, member_t_ref, send, arrive, side_send, side_arrive, local, loaded = refs
    step = pl.program_id(0)
    pairs = (pl.num_programs(0) - 1) // 2
    group, mine, across_bits = neighbours(count)
    core = lax.axis_index("mp")
    twin = (group, 1 - core)

    def view(ref, chosen, columns):
        place = tuple(chosen[b] for b in sorted(chosen, reverse=True))
        return ref.at[place + (slice(None), columns)]

    def part_view(index):
        piece, low_edge, high_edge, order = streams[index]
        done = {b: slice(None) for b in order[:-2]}
        return view(parts[piece], done, slice(low_edge, high_edge))

    def placed(ref, index, place, received):
        piece, low_edge, high_edge, order = streams[index]
        chosen = {b: slice(None) if b in order[:place] else mine[b] for b in range(count)}
        if received:
            chosen[order[place]] = 1 - mine[order[place]]
        return view(ref, chosen, slice(low_edge, high_edge))

    def hop(index, turn):
        piece, low_edge, high_edge, order = streams[index]
        place = count - 2 + turn
        target = placed(owns[piece], index, place, False)
        source = part_view(index) if turn == 0 else target
        return remote(
            source, target, send.at[index, turn], arrive.at[index, turn],
            (across_bits[order[place]], core),
        )

    def load(piece):
        return pltpu.make_async_copy(parts[piece], held[piece], loaded.at[piece])

    def settle(index):
        piece, low_edge, high_edge, order = streams[index]
        done = {b: slice(None) for b in order[:-2]}
        return pltpu.make_async_copy(
            view(held[piece], done, slice(low_edge, high_edge)), placed(owns[piece], index, count - 2, False), local.at[index]
        )

    def forward(index, turn):
        piece = streams[index][0]
        if turn == 0:
            source = part_view(index)
            target = placed(others[piece], index, count - 2, False)
        else:
            source = placed(owns[piece], index, count - 3 + turn, True)
            target = placed(others[piece], index, count - 3 + turn, True)
        return remote(
            source, target, side_send.at[index, turn], side_arrive.at[index, turn], twin
        )

    everyone = range(len(streams))

    @pl.when(step == 0)
    def _():
        enter(group, across_bits, core)
        for index in everyone:
            hop(index, 0).start()
        for piece in range(pieces):
            load(piece).start()
        for index in everyone:
            forward(index, 0).start()
        slots = valid_ref.shape[1]
        length = lengths_ref[group * lax.axis_size("mp") + core]
        member_ref[...] = membership(length, slots, False).astype(BF)
        member_t = membership(length, slots, True)
        member_t_ref[...] = member_t.astype(BF)
        share_ref[...] = 1.0 / jnp.sum(member_t, axis=0, keepdims=True)
        valid_ref[...] = (lax.broadcasted_iota(jnp.int32, (1, slots), 1) < length).astype(F32)
        tokens_t_ref[...] = tokens_ref[...].T

    @pl.when(step == 1)
    def _():
        for piece in range(pieces):
            load(piece).wait()
        for index in everyone:
            settle(index).start()

    @pl.when(step == GATHER_WHEN[0])
    def _():
        for index in everyone:
            settle(index).wait()
        for index in everyone:
            hop(index, 0).wait_recv()
            hop(index, 1).start()
            forward(index, 1).start()

    @pl.when(step == GATHER_WHEN[1])
    def _():
        for index in everyone:
            hop(index, 1).wait_recv()
            forward(index, 2).start()

    def project(weights, place):
        side = pl.ds(pl.multiple_of(step * 2 * HEAD_DIM, 2 * HEAD_DIM), 2 * HEAD_DIM)
        columns = pl.ds(pl.multiple_of(place * 2 * HEAD_DIM, 2 * HEAD_DIM), 2 * HEAD_DIM)
        for weight, ref in zip(weights, (q_ref, k_ref, v_ref)):
            ref[side, :] = tn(weight[:, columns], tokens_t_ref[...]).astype(BF)

    @pl.when(step < pairs // 2)
    def _():
        project(own_weights, step)

    @pl.when(jnp.logical_and(step >= pairs // 2, step < pairs))
    def _():
        project(other_weights, step - pairs // 2)

    @pl.when(step < pairs)
    def _():
        side = pl.ds(pl.multiple_of(step * 2 * HEAD_DIM, 2 * HEAD_DIM), 2 * HEAD_DIM)
        marks_kernel(
            q_ref.at[side, :], k_ref.at[side, :], member_t_ref, share_ref, mq_ref.at[side, :], mk_ref.at[side, :],
            a_ref.at[:, side], at_ref.at[:, side], start_ref.at[:, side],
        )

    @pl.when(step == pairs)
    def _():
        inverse_kernel(groups, a_ref, start_ref, z_ref, kept_ref)

    @pl.when(step > pairs)
    def _():
        place = step - pairs - 1
        side = pl.ds(pl.multiple_of(place * 2 * HEAD_DIM, 2 * HEAD_DIM), 2 * HEAD_DIM)
        forward_kernel(
            q_ref.at[side, :], k_ref.at[side, :], v_ref.at[side, :], mq_ref.at[side, :], mk_ref.at[side, :], z_ref.at[:, side],
            valid_ref, row_ref, out_ref, first_ref, third_ref, summary_ref, carried_ref, padded,
        )

    @pl.when(step == 2 * pairs)
    def _():
        for index in everyone:
            for turn in range(2):
                hop(index, turn).wait_send()
            for turn in range(3):
                forward(index, turn).wait()


def attention_lead(tokens, own_weights, other_weights, taps, lengths, parts, identity):
    slots, width = tokens.shape
    pairs = width // (2 * HEAD_DIM)
    groups = width // (4 * HEAD_DIM)
    flat, tall = (LANDMARKS, width), (width, LANDMARKS)
    count = bits_of(lax.axis_size("dp"))
    blocks = [jax.ShapeDtypeStruct(p.shape[count - 2 :], p.dtype) for p in parts]
    streams = gather_streams(blocks, count, 0)
    turns = pairs + 1

    def late(i):
        return i // turns * (i % turns)

    def rows(dims, pick):
        return pl.BlockSpec(dims, lambda i: (pick(i), 0))

    big, thin = (2 * HEAD_DIM, slots), (2 * HEAD_DIM, LANDMARKS)
    anywhere = pl.BlockSpec(memory_space=pl.ANY)
    once = pl.BlockSpec(memory_space=pltpu.VMEM)
    dma = pltpu.SemaphoreType.DMA
    gathered = [shape((2,) * count + b.shape, b.dtype) for b in blocks] * 2
    outs = pl.pallas_call(
        functools.partial(lead_kernel, count, streams, groups, len(parts)),
        grid=(2 * pairs + 1,),
        in_specs=[once, pl.BlockSpec(memory_space=pltpu.SMEM)]
        + [pl.BlockSpec((2, 1, 2 * BLOCK), lambda i: (late(i), 0, 0))]
        + [once] * 6
        + [anywhere] * len(parts),
        out_specs=[once] * 3
        + [rows(big, late)] * 3
        + [rows(thin, late)] * 2
        + [once] * 10
        + [anywhere] * len(gathered),
        out_shape=[shape((width, slots), BF)] * 4
        + [shape((width, slots))] * 2
        + [shape(tall)] * 4
        + [shape(flat)] * 3
        + [
            shape((PINV_STEPS, 4) + flat), shape((width, slots), BF), shape((LANDMARKS, slots), BF),
            shape((1, LANDMARKS)), shape((1, slots)),
        ]
        + gathered,
        scratch_shapes=[pltpu.VMEM(p.shape, p.dtype) for p in parts]
        + [pltpu.VMEM(flat, F32), pltpu.VMEM((HEAD_DIM, slots + MARGIN + BLOCK), BF)]
        + [pltpu.VMEM((slots, LANDMARKS), BF)]
        + [dma((len(streams), 2))] * 2
        + [dma((len(streams), 3))] * 2
        + [dma((len(streams),)), dma((len(parts),))],
        name="lead",
        compiler_params=pltpu.CompilerParams(
            collective_id=identity, has_side_effects=True, vmem_limit_bytes=62 * 1024 * 1024
        ),
        cost_estimate=cost_of(2e10, 3e7),
    )(
        tokens, lengths, tap_rows(taps, False), *own_weights, *other_weights, *parts,
    )
    q, k, v, out, first, third, summary, carried, mq, mk, a, at, z, kept = outs[:14]
    flat_outs = [o.reshape((-1,) + o.shape[count:]) for o in outs[18:]]
    pieces = list(zip(flat_outs[: len(parts)], flat_outs[len(parts) :]))
    saved = (mq, mk, a, at, z, kept, first, third, summary, carried)
    return (q, k, v), out, saved, outs[14:18], pieces


def halving(streams, bits, sums, inbox, send, arrive, across_bits, mine, core, sources=None):
    def columns_of(index):
        return (slice(None), slice(streams[index][1], streams[index][2]))

    def hop(index, place):
        piece, low_edge, high_edge, order = streams[index]
        chosen = {b: mine[b] if b in order[:place] else slice(None) for b in bits[index]}
        chosen[order[place]] = 1 - mine[order[place]]
        held = sources if sources is not None and place == 0 else sums
        source = held[piece].at[tuple(chosen[b] for b in bits[index][::-1]) + columns_of(index)]
        box = inbox[piece][place]
        lead = (slice(None),) * (len(bits[index]) - 1 - place)
        return remote(
            source, box.at[lead + columns_of(index)], send.at[index, place],
            arrive.at[index, place], (across_bits[order[place]], core),
        )

    def add(index, place, half, box):
        piece, low_edge, high_edge, order = streams[index]
        columns = columns_of(index)
        names = bits[index][::-1]
        left = [b for b in bits[index] if b not in order[: place + 1]]
        turn = mine[order[place]] if half else 1 - mine[order[place]]

        def body(i, carry):
            at = {b: mine[b] for b in names}
            at[order[place]] = turn
            for spot, b in enumerate(left):
                at[b] = (i // 2**spot) % 2
            here = tuple(at[b] for b in names)
            there = tuple(at[b] for b in names if b not in order[:place])
            there = here if len(box.shape) == len(here) + 2 else there
            value = sums[piece][here + columns].astype(F32) + box[there + columns].astype(F32)
            sums[piece][here + columns] = value.astype(BF)
            return carry

        lax.fori_loop(0, 2 ** len(left), body, 0)

    return hop, add


def scatter_kernel(count, streams, bits, joined, settled, *refs):
    pieces = len(joined)
    depth = {stream[0]: len(bits[index]) for index, stream in enumerate(streams)}
    owns, refs = refs[:pieces], refs[pieces:]
    others, refs = refs[:pieces], refs[pieces:]
    small_ref, refs = refs[0], refs[1:]
    grads, refs = refs[:3], refs[3:]
    weights, refs = refs[:6], refs[6:]
    results, refs = refs[:pieces], refs[pieces:]
    (total_ref, back_ref), refs = refs[:2], refs[2:]
    sums, refs = refs[:pieces], refs[pieces:]
    twins, refs = refs[:pieces], refs[pieces:]
    inbox = []
    for piece in range(pieces):
        inbox.append(refs[: depth[piece]])
        refs = refs[depth[piece] :]
    small_sum, small_in, send, arrive, side_send, side_arrive, local, small_send, small_arrive = refs
    group, mine, across_bits = neighbours(count)
    core = lax.axis_index("mp")
    twin = (group, 1 - core)
    hop, add = halving(streams, bits, sums, inbox, send, arrive, across_bits, mine, core)
    enter(group, across_bits, core)

    def small_hop(place):
        if place == 0:
            return remote(small_ref, small_in.at[0], small_send.at[0], small_arrive.at[0], twin)
        return remote(
            small_sum.at[place - 1], small_in.at[place], small_send.at[place],
            small_arrive.at[place], (across_bits[place - 1], core),
        )

    small = [small_hop(0)]
    small[0].start()
    starts = []
    for index, (piece, low_edge, high_edge, order) in enumerate(streams):
        lead, tail = (slice(None),) * len(bits[index]), (slice(None), slice(low_edge, high_edge))
        place = lead + tail
        own_place = other_place = place
        if joined[piece] == "rows":
            own_place, other_place = lead + (core,) + tail, lead + (1 - core,) + tail
        if joined[piece] == "columns":
            size = owns[piece].shape[-1] // 2
            other_place = lead + (slice(None), slice(size + low_edge, size + high_edge))
        copy = pltpu.make_async_copy(
            owns[piece].at[own_place], sums[piece].at[place], local.at[index]
        )
        copy.start()
        side = None
        if not settled[piece]:
            side = remote(
                others[piece].at[other_place], twins[piece].at[place], side_send.at[index],
                side_arrive.at[index], twin,
            )
            side.start()
        starts.append((copy, side))

    def back(first, last):
        size = weights[0].shape[1]
        for tile in range(first, last):
            rows = slice(tile * 128, (tile + 1) * 128)
            total = jnp.zeros((128, back_ref.shape[0]), F32)
            for i, weight in enumerate(weights):
                half = slice(i // 3 * size, (i // 3 + 1) * size)
                total = total + nn(weight[rows, :], grads[i % 3][half, :])
            back_ref[:, rows] = total.T

    tiles = back_ref.shape[1] // 128
    hops = [[] for stream in streams]
    for place in range(count):
        back(tiles * place // (count + 1), tiles * (place + 1) // (count + 1))
        small[place].wait_recv()
        before = small_ref[...] if place == 0 else small_sum[place - 1]
        small_sum[place] = before + small_in[place]
        small.append(small_hop(place + 1))
        small[place + 1].start()
        for index, (piece, low_edge, high_edge, order) in enumerate(streams):
            if place >= len(order):
                continue
            box = twins[piece] if place == 0 else inbox[piece][place - 1]
            if place == 0:
                copy, side = starts[index]
                copy.wait()
                if side is not None:
                    side.wait_recv()
            else:
                hops[index][place - 1].wait_recv()
            if place > 0 or side is not None:
                add(index, place, 0, box)
            one = hop(index, place)
            one.start()
            hops[index].append(one)
            if place > 0 or side is not None:
                add(index, place, 1, box)
    back(tiles * count // (count + 1), tiles)
    small[count].wait_recv()
    total_ref[...] = small_sum[count - 1] + small_in[count]
    for index, (piece, low_edge, high_edge, order) in enumerate(streams):
        hops[index][-1].wait_recv()
        columns = (slice(None), slice(low_edge, high_edge))
        results[piece][columns] = (
            sums[piece][tuple(mine[b] for b in bits[index][::-1]) + columns].astype(F32)
            + inbox[piece][-1][columns].astype(F32)
        )
    for copy, side in starts:
        if side is not None:
            side.wait_send()
    for one in small:
        one.wait_send()
    for line in hops:
        for one in line:
            one.wait_send()


def scatter(owns, others, small, grads, weights, identity):
    groups = lax.axis_size("dp")
    count = bits_of(groups)
    settled = [other is None for other in others]
    joined = [
        "rows" if own.ndim == 4 else "columns" if own is other else ""
        for own, other in zip(owns, others)
    ]
    shapes = [
        (b.shape[-2], b.shape[-1] // 2 if how == "columns" else b.shape[-1])
        for b, how in zip(owns, joined)
    ]
    depths = [bits_of(b.shape[0]) for b in owns]
    streams = [
        (piece, low_edge, high_edge, order[count - depths[piece] :])
        for piece, low_edge, high_edge, order in colored(
            [dims[-1] for dims in shapes], scatter_orders(count)
        )
    ]
    bits = [sorted(stream[3]) for stream in streams]
    leads = [(2,) * depth for depth in depths]
    dma = pltpu.SemaphoreType.DMA
    vmem = pl.BlockSpec(memory_space=pltpu.VMEM)
    others = [own if other is None else other for own, other in zip(owns, others)]
    outs = pl.pallas_call(
        functools.partial(scatter_kernel, count, streams, bits, joined, settled),
        in_specs=[pl.BlockSpec(memory_space=pl.ANY)] * (2 * len(owns)) + [vmem] * 10,
        out_specs=[vmem] * (len(owns) + 2),
        out_shape=[jax.ShapeDtypeStruct(s, F32) for s in shapes]
        + [
            jax.ShapeDtypeStruct(small.shape, F32),
            jax.ShapeDtypeStruct((grads[0].shape[1], weights[0].shape[0]), F32),
        ],
        scratch_shapes=[pltpu.VMEM(lead + s, BF) for lead, s in zip(leads, shapes)]
        + [
            pltpu.VMEM((8, 128) if done else lead + s, BF)
            for lead, s, done in zip(leads, shapes, settled)
        ]
        + [
            pltpu.VMEM(lead[: len(lead) - 1 - place] + s, BF)
            for lead, s in zip(leads, shapes)
            for place in range(len(lead))
        ]
        + [pltpu.VMEM((count,) + small.shape, F32), pltpu.VMEM((count + 1,) + small.shape, F32)]
        + [dma((len(streams), count))] * 2
        + [dma((len(streams),))] * 3
        + [dma((count + 1,))] * 2,
        name="scatter",
        compiler_params=pltpu.CompilerParams(
            collective_id=identity, has_side_effects=True, vmem_limit_bytes=62 * 1024 * 1024
        ),
    )(
        *[
            b.reshape(lead + b.shape[1:])
            for b, lead in zip(owns + others, leads + leads)
        ],
        small,
        *grads,
        *weights,
    )
    return outs[:-2], outs[-2], outs[-1]


def tail_kernel(count, streams, bits, groups, pieces, *refs):
    (
        d_ref, q_ref, k_ref, v_ref, first_ref, third_ref, mq_ref, mk_ref, carried_ref, a_ref,
        at_ref, z_ref, kept_ref, summary_ref, member_ref, share_ref, valid_ref, row_ref, tokens_ref,
    ), refs = refs[:19], refs[19:]
    sources, refs = refs[:pieces], refs[pieces:]
    (dq_ref, dk_ref, dv_ref, taps_ref), refs = refs[:4], refs[4:]
    weight_grads, refs = refs[:3], refs[3:]
    results, refs = refs[:pieces], refs[pieces:]
    (gz_ref, dsum_ref, ds_ref, padded), refs = refs[:4], refs[4:]
    sums, refs = refs[:pieces], refs[pieces:]
    hop_count = len(streams[0][3])
    inbox = []
    for piece in range(pieces):
        inbox.append(refs[:hop_count])
        refs = refs[hop_count:]
    send, arrive, local, store = refs
    step = pl.program_id(0)
    pairs = (pl.num_programs(0) - 1) // 2
    group, mine, across_bits = neighbours(count)
    core = lax.axis_index("mp")
    hop, add = halving(
        streams, bits, sums, inbox, send, arrive, across_bits, mine, core, sources
    )

    def load(piece):
        return pltpu.make_async_copy(sources[piece], sums[piece], local.at[piece])

    def save(index):
        piece, low_edge, high_edge, order = streams[index]
        columns = (slice(None), slice(low_edge, high_edge))
        spot = tuple(slice(None) if b not in order else mine[b] for b in bits[index][::-1])
        lead = (slice(None),) * (count - hop_count)
        return pltpu.make_async_copy(
            sums[piece].at[spot + columns], results[piece].at[lead + columns], store.at[index]
        )

    @pl.when(step == 0)
    def _():
        enter(group, across_bits, core)
        for index in range(len(streams)):
            hop(index, 0).start()
        for piece in range(pieces):
            load(piece).start()

    def add_last(index, box):
        piece, low_edge, high_edge, order = streams[index]
        columns = (slice(None), slice(low_edge, high_edge))
        left = [b for b in bits[index] if b not in order]

        def body(i, carry):
            at = {b: mine[b] for b in bits[index]}
            for spot, b in enumerate(left):
                at[b] = (i // 2**spot) % 2
            here = tuple(at[b] for b in bits[index][::-1])
            there = tuple(at[b] for b in bits[index][::-1] if b in left)
            value = sums[piece][here + columns].astype(F32) + box[there + columns].astype(F32)
            sums[piece][here + columns] = value.astype(BF)
            return carry

        lax.fori_loop(0, 2 ** len(left), body, 0)

    for place in range(1, hop_count + 1):

        @pl.when(step == WHEN[place])
        def _():
            if place == 1:
                for piece in range(pieces):
                    load(piece).wait()
            for index, (piece, low_edge, high_edge, order) in enumerate(streams):
                hop(index, place - 1).wait_recv()
                box = inbox[piece][place - 1]
                if place < hop_count:
                    add(index, place, 0, box)
                    hop(index, place).start()
                    add(index, place, 1, box)
                else:
                    add_last(index, box)

    @pl.when(step < pairs)
    def _():
        side = pl.ds(pl.multiple_of(step * 2 * HEAD_DIM, 2 * HEAD_DIM), 2 * HEAD_DIM)
        carried_back_kernel(
            d_ref, first_ref, z_ref, summary_ref, valid_ref, gz_ref.at[:, side],
            dsum_ref.at[side, :],
        )

    @pl.when(step == pairs)
    def _():
        inverse_back_kernel(groups, a_ref, at_ref, kept_ref, gz_ref, ds_ref)

    @pl.when(step > pairs)
    def _():
        place = step - pairs - 1
        side = pl.ds(pl.multiple_of(place * 2 * HEAD_DIM, 2 * HEAD_DIM), 2 * HEAD_DIM)
        backward_kernel(
            d_ref, q_ref, k_ref, v_ref, first_ref, third_ref, mq_ref, mk_ref, carried_ref,
            dsum_ref.at[side, :], ds_ref.at[:, side], member_ref, share_ref, valid_ref, row_ref,
            dq_ref, dk_ref, dv_ref, taps_ref, padded,
        )
        for grad, ref in zip((dq_ref, dk_ref, dv_ref), weight_grads):
            ref[...] = nt(tokens_ref[...], grad[...]).astype(BF)

    @pl.when(step == 2 * pairs)
    def _():
        for index in range(len(streams)):
            save(index).start()
        for index in range(len(streams)):
            for place in range(hop_count):
                hop(index, place).wait_send()
        for index in range(len(streams)):
            save(index).wait()


def attention_tail(d, q, k, v, taps, setup, saved, grads, identity):
    mq, mk, a, at, z, kept, first, third, summary, carried = saved
    width, slots = q.shape
    pairs = width // (2 * HEAD_DIM)
    groups = width // (4 * HEAD_DIM)
    tokens_t, member, share, valid = setup
    flat = (LANDMARKS, width)
    count = bits_of(lax.axis_size("dp"))
    hop_count = min(3, count - 1)
    streams = [
        (piece, low_edge, high_edge, order[:hop_count])
        for piece, low_edge, high_edge, order in colored(
            [b.shape[-1] for b in grads], scatter_orders(count)
        )
    ]
    bits = [list(range(count))] * len(streams)
    lead = (2,) * count
    shapes = [b.shape[1:] for b in grads]
    turns = pairs + 1

    def both(i):
        return i % turns - i % turns // pairs

    def late(i):
        return i // turns * (i % turns)

    def early(i):
        return both(i) * (1 - i // turns) + (pairs - 1) * (i // turns)

    def spec(dims, index):
        return pl.BlockSpec(dims, index)

    big, tall, side = (2 * HEAD_DIM, slots), (2 * HEAD_DIM, LANDMARKS), (LANDMARKS, 2 * LANDMARKS)

    def rows(dims, pick):
        return spec(dims, lambda i: (pick(i), 0))

    anywhere = pl.BlockSpec(memory_space=pl.ANY)
    once = pl.BlockSpec(memory_space=pltpu.VMEM)
    dma = pltpu.SemaphoreType.DMA
    outs = pl.pallas_call(
        functools.partial(tail_kernel, count, streams, bits, groups, len(grads)),
        grid=(2 * pairs + 1,),
        in_specs=[
            rows(big, both), rows(big, late), rows(big, late), rows(big, late), rows(big, both),
            rows(big, late), rows(tall, late), rows(tall, late), rows(tall, late), once, once,
            spec(side, lambda i: (0, early(i))), once, rows(tall, early), once, once, once,
            spec((2, 1, 2 * BLOCK), lambda i: (late(i), 0, 0)), once,
        ]
        + [anywhere] * len(grads),
        out_specs=[rows(big, late)] * 3
        + [spec((2, 1, 384), lambda i: (late(i), 0, 0))]
        + [spec((width, 2 * HEAD_DIM), lambda i: (0, late(i)))] * 3
        + [anywhere] * len(grads),
        out_shape=[shape(q.shape, BF)] * 3
        + [shape((2 * pairs, 1, 384))]
        + [shape((width, width), BF)] * 3
        + [shape((2,) * (count - hop_count) + s, BF) for s in shapes],
        scratch_shapes=[
            pltpu.VMEM(flat, F32), pltpu.VMEM((width, LANDMARKS), F32), pltpu.VMEM(flat, F32),
            pltpu.VMEM((HEAD_DIM, slots + MARGIN + BLOCK), BF),
        ]
        + [pltpu.VMEM(lead + s, BF) for s in shapes]
        + [
            pltpu.VMEM(lead[: count - 1 - place] + s, BF)
            for s in shapes
            for place in range(hop_count)
        ]
        + [dma((len(streams), hop_count))] * 2
        + [dma((len(grads),)), dma((len(streams),))],
        name="tail",
        compiler_params=pltpu.CompilerParams(
            collective_id=identity, has_side_effects=True, vmem_limit_bytes=62 * 1024 * 1024
        ),
        cost_estimate=cost_of(4e10, 4e7),
    )(
        d, q, k, v, first, third, mq, mk, carried, a, at, z, kept, summary, member, share, valid,
        tap_rows(taps, True), tokens_t, *[b.reshape(lead + b.shape[1:]) for b in grads],
    )
    dq, dk, dv, spread = outs[:4]
    sums = [o.reshape((-1,) + s) for o, s in zip(outs[7:], shapes)]
    start = 2 * MARGIN - 1 - KERNEL // 2
    return (dq, dk, dv), spread[:, 0, start : start + KERNEL], outs[4:7], sums


def normed(values):
    centered = values - jnp.mean(values, axis=1, keepdims=True)
    scale = lax.rsqrt(jnp.mean(centered * centered, axis=1, keepdims=True) + 1e-05)
    return centered * scale, scale


def normed_back(grad, unit, scale):
    return scale * (
        grad
        - jnp.mean(grad, axis=1, keepdims=True)
        - unit * jnp.mean(grad * unit, axis=1, keepdims=True)
    )


def middle_kernel(
    chunk, att_ref, tokens_ref, grad_ref, output_ref, e_own_ref, e_oth_ref, s_own_ref, s_oth_ref,
    norms_ref, out_ref, first_in_ref, branch_ref, hidden_ref, act_own_ref, act_oth_ref,
    pre_own_ref, pre_oth_ref, projected_ref, attended_ref, small_ref, slope_ref,
):
    gain_one, bias_one, gain_two, bias_two = (norms_ref[i : i + 1, :] for i in range(4))
    projected = nn(output_ref[...], att_ref[...]).T
    unit_one, scale_one = normed(tokens_ref[...].astype(F32) + projected)
    first_out = unit_one * gain_one + bias_one
    hidden_in = first_out.astype(BF)
    hidden_ref[...] = hidden_in
    size = e_own_ref.shape[1]
    total = first_out
    sides = ((e_own_ref, s_own_ref, act_own_ref), (e_oth_ref, s_oth_ref, act_oth_ref))
    for side, (e_ref, s_ref, act_ref) in enumerate(sides):
        for start in range(0, size, chunk):
            part = slice(start, start + chunk)
            pre = nn(hidden_in, e_ref[:, part])
            share = 0.5 * (1.0 + lax.erf(pre * 0.7071067811865476))
            density = jnp.exp(-0.5 * pre * pre) * 0.3989422804014327
            active = (pre * share).astype(BF)
            act_ref[:, part] = active
            slope_ref[:, side * size + start : side * size + start + chunk] = (
                share + pre * density
            )
            total = total + nt(active, s_ref[:, part])
    unit_two, scale_two = normed(total)
    out_ref[...] = (unit_two * gain_two + bias_two).astype(BF)
    grad = grad_ref[...].astype(F32)
    second_in = normed_back(grad * gain_two, unit_two, scale_two)
    d_branch = second_in.astype(BF)
    branch_ref[...] = d_branch
    first_grad = second_in
    sides = ((e_own_ref, s_own_ref, pre_own_ref), (e_oth_ref, s_oth_ref, pre_oth_ref))
    for side, (e_ref, s_ref, pre_ref) in enumerate(sides):
        for start in range(0, size, chunk):
            part = slice(start, start + chunk)
            d_pre = (
                nn(d_branch, s_ref[:, part])
                * slope_ref[:, side * size + start : side * size + start + chunk]
            ).astype(BF)
            pre_ref[:, part] = d_pre
            first_grad = first_grad + nt(d_pre, e_ref[:, part])
    first_in = normed_back(first_grad * gain_one, unit_one, scale_one)
    first_in_ref[...] = first_in
    d_projected = first_in.astype(BF)
    projected_ref[...] = d_projected
    attended_ref[...] = nn(d_projected, output_ref[...]).T.astype(BF)
    sums = jnp.concatenate(
        [
            jnp.sum(x, axis=0, keepdims=True)
            for x in (first_grad * unit_one, first_grad, grad * unit_two, grad)
        ],
        axis=0,
    )

    @pl.when(pl.program_id(0) == 0)
    def _():
        small_ref[...] = sums

    @pl.when(pl.program_id(0) > 0)
    def _():
        small_ref[...] += sums


def middle(att, tokens, grad, output_t, e_own, e_oth, s_own, s_oth, norms):
    slots, width = tokens.shape
    size = e_own.shape[1]
    tile = TILE
    once = pl.BlockSpec(memory_space=pltpu.VMEM)

    def rows(columns):
        return pl.BlockSpec((tile, columns), lambda i: (i, 0))

    across_tile = pl.BlockSpec((width, tile), lambda i: (0, i))
    return call(
        functools.partial(middle_kernel, CHUNK if size % CHUNK == 0 else size), (slots // tile,),
        [across_tile, rows(width), rows(width)] + [once] * 6,
        [rows(width)] * 4 + [rows(size)] * 4 + [rows(width), across_tile, fixed((4, width))],
        [
            shape((slots, width), BF), shape((slots, width)), shape((slots, width), BF),
            shape((slots, width), BF),
        ]
        + [shape((slots, size), BF)] * 4
        + [shape((slots, width), BF), shape((width, slots), BF), shape((4, width))],
        "middle", [pltpu.VMEM((tile, 2 * size), F32)], cost=cost_of(2.2e10, 4e7),
    )(att, tokens, grad, output_t, e_own, e_oth, s_own, s_oth, norms)


def on_device(
    tokens,
    w_query,
    w_key,
    w_value,
    value_taps,
    w_output,
    first_gain,
    first_bias,
    w_expand,
    w_shrink,
    second_gain,
    second_bias,
    doc_lengths,
    out_grad,
):
    parts = lax.axis_size("mp")
    groups = lax.axis_size("dp")
    group = lax.axis_index("dp")
    core = lax.axis_index("mp")
    slots, width = tokens.shape
    half = w_query.shape[1]
    hidden_half = w_expand.shape[1]
    rows = w_query.shape[0]

    def in_core_order(own, other, axis):
        return jnp.where(
            core == 0,
            jnp.concatenate([own, other], axis=axis),
            jnp.concatenate([other, own], axis=axis),
        )

    sides = rows // parts
    own_heads = value_taps.shape[0]
    notes = jnp.pad(value_taps, ((8, 8 - own_heads), (0, 128 - KERNEL)))
    for row, norm in enumerate((first_gain, first_bias, second_gain, second_bias)):
        notes = notes + jnp.pad(wide(norm)[None], ((row, 15 - row), (0, 128 - sides)))
    heads, hidden_parts = gather(
        [w_query, w_key, w_value, w_output.T, notes], [w_expand, w_shrink.T], 0
    )
    (out_own, out_other), (note_own, note_other) = heads[3:]
    output_t = in_core_order(out_own[:, None], out_other[:, None], 1).reshape(width, width)
    output_t = jnp.where(
        core == 0, output_t, jnp.concatenate([output_t[:, half:], output_t[:, :half]], axis=1)
    )
    norms = in_core_order(note_own[:, None, :4, :sides], note_other[:, None, :4, :sides], 1)
    norms = norms.transpose(2, 0, 1, 3).reshape(4, width)
    other_taps = lax.dynamic_index_in_dim(note_other, group, 0, keepdims=False)
    taps = jnp.concatenate([value_taps, other_taps[8 : 8 + own_heads, :KERNEL]], axis=0)

    def flat(pair):
        return pair[0].reshape(width, -1), pair[1].reshape(width, -1)

    (q_own, q_oth), (k_own, k_oth), (v_own, v_oth) = (flat(pair) for pair in heads[:3])

    own_weights, other_weights = [q_own, k_own, v_own], [q_oth, k_oth, v_oth]
    (query, keys, values), attended, saved, setup, hiddens = attention_lead(
        tokens, own_weights, other_weights, taps, doc_lengths, hidden_parts, 3
    )
    (e_own, e_oth), (s_own, s_oth) = (flat(pair) for pair in hiddens)
    (
        layer_out, d_first_in, d_branch, hidden_in, act_own, act_oth, d_pre_own, d_pre_oth,
        d_projected, d_attended, norm_sums,
    ) = middle(attended, tokens, out_grad, output_t, e_own, e_oth, s_own, s_oth, norms)

    def blocks(values):
        return low(values).reshape(groups, rows, values.shape[1])

    shrink_got = partner(low(across(d_branch, act_oth)))
    expand_got = partner(low(across(hidden_in, d_pre_oth)))
    shrink_sum = blocks(across(d_branch, act_own) + wide(shrink_got))
    expand_sum = blocks(across(hidden_in, d_pre_own) + wide(expand_got))
    head_grads, taps_grad, weight_grads, (shrink_part, expand_part) = attention_tail(
        d_attended, query, keys, values, taps, setup, saved, [shrink_sum, expand_sum], 2
    )
    output_part = in_core_order(
        low(crossed(d_projected, attended[:half])), low(crossed(d_projected, attended[half:])), 1
    ).reshape(groups, parts, sides, width)
    taps_grad = in_core_order(taps_grad[:own_heads], taps_grad[own_heads:], 0)
    small = jnp.concatenate(
        [
            norm_sums,
            jnp.pad(taps_grad, ((0, 12 - taps_grad.shape[0]), (0, width - KERNEL))),
        ],
        axis=0,
    )
    query_part, keys_part, values_part = (
        grad.reshape(groups, rows, width) for grad in weight_grads
    )
    pieces = [shrink_part, expand_part, query_part, keys_part, values_part, output_part]
    sums, small, back = scatter(
        pieces, [None, None] + pieces[2:], small, head_grads, own_weights + other_weights, 1
    )
    shrink_grad, expand_grad, query_grad, key_grad, value_grad, output_grad = sums
    tokens_grad = d_first_in + back
    taps_grad = lax.dynamic_slice(small, (4 + core * own_heads, 0), (own_heads, KERNEL))
    norm_grads = lax.dynamic_slice(small, (0, group * rows + core * sides), (4, sides))
    return (
        layer_out,
        tokens_grad,
        query_grad,
        key_grad,
        value_grad,
        taps_grad,
        output_grad.T,
        norm_grads[0],
        norm_grads[1],
        expand_grad,
        shrink_grad.T,
        norm_grads[2],
        norm_grads[3],
    )


def solution(mesh):
    tokens_spec = P(("dp", "mp"), None)
    vector = P(("dp", "mp"))
    in_specs = (
        tokens_spec,
        P("dp", "mp"),
        P("dp", "mp"),
        P("dp", "mp"),
        P("mp", None),
        P(None, ("dp", "mp")),
        vector,
        vector,
        P("dp", "mp"),
        P("mp", "dp"),
        vector,
        vector,
        P(),
        tokens_spec,
    )
    out_specs = (
        tokens_spec,
        tokens_spec,
        P("dp", "mp"),
        P("dp", "mp"),
        P("dp", "mp"),
        P("mp", None),
        P(None, ("dp", "mp")),
        vector,
        vector,
        P("dp", "mp"),
        P("mp", "dp"),
        vector,
        vector,
    )
    return jax.shard_map(
        on_device, mesh=mesh, in_specs=in_specs, out_specs=out_specs, check_vma=False
    )
```

```python
import functools
import jax
import jax.numpy as jnp
from jax import lax
from jax.experimental import pallas as pl
from jax.experimental.pallas import tpu as pltpu
from jax.sharding import PartitionSpec as P

HEAD_DIM = 64
LANDMARKS = 64
KERNEL = 33
PINV_STEPS = 6
HIGH = lax.Precision.HIGHEST
SCALE = HEAD_DIM ** (-0.5)
BLOCK = 256
MARGIN = 128
WHEN = (0, 7, 10, 12)
GATHER_WHEN = (5, 11)
TILE = 512
CHUNK = 256
BF = jnp.bfloat16
F32 = jnp.float32


def nn(left, right, precision=None):
    return lax.dot_general(left, right, (((1,), (0,)), ((), ())), precision=precision, preferred_element_type=F32)


def nt(left, right, precision=None):
    return lax.dot_general(left, right, (((1,), (1,)), ((), ())), precision=precision, preferred_element_type=F32)


def tn(left, right, precision=None):
    return lax.dot_general(left, right, (((0,), (0,)), ((), ())), precision=precision, preferred_element_type=F32)


def split(values):
    high = values.astype(BF)
    return high, (values - high.astype(F32)).astype(BF)


def exact_left(left, right):
    high, rest = split(left)
    return nn(jnp.concatenate([high, rest], axis=1), jnp.concatenate([right, right], axis=0))


def once_both(left, right):
    return nn(left.astype(BF), right.astype(BF))


def exact_both(left, right):
    high, rest = split(left)
    right_high, right_rest = split(right)
    return nn(
        jnp.concatenate([high, rest, high], axis=1),
        jnp.concatenate([right_high, right_high, right_rest], axis=0),
    )


def exact_rows(left, right):
    high, rest = split(left)
    both = nt(jnp.concatenate([high, rest], axis=0), right)
    return both[: left.shape[0]] + both[left.shape[0] :]


def band(row):
    spread = jnp.broadcast_to(row, (2 * BLOCK, 2 * BLOCK))
    return pltpu.roll(spread, 0, 1, stride=1, stride_axis=0)[:, :BLOCK]


def convolve(values, row, padded):
    slots = values.shape[1]
    padded[...] = jnp.zeros(padded.shape, BF)
    padded[:, MARGIN : MARGIN + slots] = values
    windows = jnp.concatenate(
        [padded[:, b * BLOCK : (b + 2) * BLOCK] for b in range(slots // BLOCK)], axis=0
    )
    high, rest = split(band(row))
    result = nn(windows, high) + nn(windows, rest)
    d = values.shape[0]
    return jnp.concatenate(
        [result[b * d : (b + 1) * d] for b in range(slots // BLOCK)], axis=1
    )


def marks_kernel(q_ref, k_ref, member_t_ref, share_ref, mq_ref, mk_ref, a_ref, at_ref, z_ref):
    mq = nn(q_ref[...], member_t_ref[...]) * share_ref[...]
    mk = nn(k_ref[...], member_t_ref[...]) * share_ref[...]
    mq_ref[...] = mq
    mk_ref[...] = mk
    firsts, seconds, starts = [], [], []
    for h in range(2):
        part = slice(h * HEAD_DIM, (h + 1) * HEAD_DIM)
        scores = tn(mk[part], mq[part], HIGH) * SCALE
        grown = jnp.exp(scores - jnp.max(scores, axis=0, keepdims=True))
        second_t = grown / jnp.sum(grown, axis=0, keepdims=True)
        second = second_t.T
        widest = jnp.max(jnp.sum(second, axis=0, keepdims=True), axis=1, keepdims=True)
        firsts.append(second)
        seconds.append(second_t)
        starts.append(second_t / widest)
    a_ref[...] = jnp.concatenate(firsts, axis=1)
    at_ref[...] = jnp.concatenate(seconds, axis=1)
    z_ref[...] = jnp.concatenate(starts, axis=1)


def diagonal(values, mask):
    return jnp.where(mask, jnp.concatenate([values] * 4, axis=0), jnp.zeros((), BF))


def group_product(left, right, mask):
    high, rest = split(left)
    right_high, right_rest = split(right)
    both = nn(jnp.concatenate([high, rest], axis=0), diagonal(right_high, mask))
    return both[:LANDMARKS] + both[LANDMARKS:] + nn(high, diagonal(right_rest, mask))


def group_mask():
    width = 4 * LANDMARKS
    return (
        lax.broadcasted_iota(jnp.int32, (width, width), 0) // LANDMARKS
        == lax.broadcasted_iota(jnp.int32, (width, width), 1) // LANDMARKS
    )


def group_identity():
    shape = (LANDMARKS, 4 * LANDMARKS)
    return (
        lax.broadcasted_iota(jnp.int32, shape, 0)
        == lax.broadcasted_iota(jnp.int32, shape, 1) % LANDMARKS
    ).astype(F32)


def inverse_kernel(groups, a_ref, z0_ref, z_ref, kept_ref):
    mask, identity = group_mask(), group_identity()
    wide = 4 * LANDMARKS
    spans = [slice(g * wide, (g + 1) * wide) for g in range(groups)]
    a = [a_ref[:, s] for s in spans]
    z = [z0_ref[:, s] for s in spans]
    for step in range(PINV_STEPS):
        p = [group_product(x, y, mask) for x, y in zip(a, z)]
        t = [15.0 * identity - group_product(x, 7.0 * identity - x, mask) for x in p]
        u = [13.0 * identity - group_product(x, y, mask) for x, y in zip(p, t)]
        for s, zz, pp, tt, uu in zip(spans, z, p, t, u):
            kept_ref[step, 0, :, s] = zz
            kept_ref[step, 1, :, s] = pp
            kept_ref[step, 2, :, s] = tt
            kept_ref[step, 3, :, s] = uu
        z = [0.25 * group_product(x, y, mask) for x, y in zip(z, u)]
    for s, zz in zip(spans, z):
        z_ref[:, s] = zz


def inverse_back_kernel(groups, a_ref, at_ref, kept_ref, gz_ref, ds_ref):
    mask, identity = group_mask(), group_identity()
    wide = 4 * LANDMARKS
    spans = [slice(g * wide, (g + 1) * wide) for g in range(groups)]
    a = [a_ref[:, s] for s in spans]
    gz = [gz_ref[:, s] for s in spans]
    ga = [jnp.zeros_like(x) for x in a]
    for step in range(PINV_STEPS)[::-1]:
        z, p, t, u = ([kept_ref[step, i, :, s] for s in spans] for i in range(4))
        gu = [0.25 * group_product(x, y, mask) for x, y in zip(gz, z)]
        gt = [-group_product(x, y, mask) for x, y in zip(gu, p)]
        g7 = [-group_product(x, y, mask) for x, y in zip(gt, p)]
        gp = [
            -group_product(tt, guu, mask) - group_product(7.0 * identity - pp, gtt, mask) - gg
            for tt, guu, pp, gtt, gg in zip(t, gu, p, gt, g7)
        ]
        ga = [x + group_product(zz, g, mask) for x, zz, g in zip(ga, z, gp)]
        gz = [
            0.25 * group_product(uu, g, mask) + group_product(gpp, aa, mask)
            for uu, g, gpp, aa in zip(u, gz, gp, a)
        ]
    for s, aa, gaa, gzz in zip(spans, a, ga, gz):
        second_t = at_ref[:, s]
        sums = jnp.sum(aa, axis=0, keepdims=True)
        pieces = []
        for h in range(4):
            part = slice(h * LANDMARKS, (h + 1) * LANDMARKS)
            start_grad = gzz[:, part].T
            column = sums[:, part]
            widest = jnp.max(column, axis=1, keepdims=True)
            chosen = (column == widest).astype(F32)
            chosen = chosen / jnp.sum(chosen, axis=1, keepdims=True)
            at_h = second_t[:, part]
            widest_grad = -jnp.sum(
                jnp.sum(start_grad * at_h, axis=0, keepdims=True), axis=1, keepdims=True
            ) / (widest * widest)
            grad = gaa[:, part] + start_grad / widest
            grad = grad + jnp.transpose(
                jnp.broadcast_to(chosen * widest_grad, (LANDMARKS, LANDMARKS))
            )
            pieces.append((grad, at_h))
        for h, (grad, at_h) in enumerate(pieces):
            inner = jnp.sum(grad * at_h, axis=0, keepdims=True)
            pieces[h] = at_h * (grad - inner) * SCALE
        ds_ref[:, s] = jnp.concatenate(pieces, axis=1)


def forward_kernel(
    q_ref, k_ref, v_ref, mq_ref, mk_ref, z_ref, valid_ref, row_ref,
    out_ref, first_ref, third_ref, summary_ref, carried_ref, padded,
):
    valid = valid_ref[...]
    for h in range(2):
        part = slice(h * HEAD_DIM, (h + 1) * HEAD_DIM)
        q, k, v = q_ref[part, :], k_ref[part, :], v_ref[part, :]
        scores = exact_left(mk_ref[part, :].T, q) * SCALE
        grown = jnp.exp(scores - jnp.max(scores, axis=0, keepdims=True))
        first = grown / jnp.sum(grown, axis=0, keepdims=True)
        first_ref[part, :] = first
        scores = exact_left(mq_ref[part, :].T, k) * SCALE
        scores = jnp.where(valid > 0.0, scores, -1e30)
        grown = jnp.exp(scores - jnp.max(scores, axis=1, keepdims=True))
        third = grown / jnp.sum(grown, axis=1, keepdims=True)
        third_ref[part, :] = third
        summary = exact_rows(third, v)
        summary_ref[part, :] = summary
        carried = nn(z_ref[:, part], summary, HIGH)
        carried_ref[part, :] = carried
        mixed = exact_both(carried.T, first)
        masked = v * valid.astype(BF)
        mixed = mixed + convolve(masked, row_ref[h], padded)
        out_ref[part, :] = (mixed * valid).astype(BF)


def carried_back_kernel(d_ref, first_ref, z_ref, summary_ref, valid_ref, gz_ref, dsum_ref):
    valid = valid_ref[...].astype(BF)
    pieces = []
    for h in range(2):
        part = slice(h * HEAD_DIM, (h + 1) * HEAD_DIM)
        d_mixed = d_ref[part, :] * valid
        d_carried = exact_rows(first_ref[part, :], d_mixed)
        dsum_ref[part, :] = nn(z_ref[:, part].T, d_carried, HIGH)
        pieces.append(nt(summary_ref[part, :], d_carried, HIGH))
    gz_ref[...] = jnp.concatenate(pieces, axis=1)


def backward_kernel(
    d_ref, q_ref, k_ref, v_ref, first_ref, third_ref, mq_ref, mk_ref, carried_ref, dsum_ref,
    ds_ref, member_ref, share_ref, valid_ref, row_ref, dq_ref, dk_ref, dv_ref, taps_ref, padded,
):
    valid = valid_ref[...]
    low_valid = valid.astype(BF)
    member = member_ref[...]
    share = share_ref[...]
    slots = valid.shape[1]
    places = (MARGIN, MARGIN)
    turn = (
        lax.broadcasted_iota(jnp.int32, places, 0) + lax.broadcasted_iota(jnp.int32, places, 1)
        == MARGIN - 1
    ).astype(F32).astype(BF)
    for h in range(2):
        part = slice(h * HEAD_DIM, (h + 1) * HEAD_DIM)
        q, k, v = q_ref[part, :], k_ref[part, :], v_ref[part, :]
        d_mixed = d_ref[part, :] * low_valid
        mq_t, mk_t = mq_ref[part, :], mk_ref[part, :]
        first, third = first_ref[part, :], third_ref[part, :]
        d_first = exact_left(carried_ref[part, :], d_mixed)
        d_scores = first * (d_first - jnp.sum(first * d_first, axis=0, keepdims=True)) * SCALE
        d_query = once_both(mk_t, d_scores)
        d_mk = exact_rows(d_scores, q).T
        d_summary = dsum_ref[part, :]
        d_third = exact_left(d_summary, v)
        d_scores = third * (d_third - jnp.sum(third * d_third, axis=1, keepdims=True)) * SCALE
        d_values = once_both(d_summary.T, third)
        d_keys = once_both(mq_t, d_scores)
        d_mq = exact_rows(d_scores, k).T
        ds_t = ds_ref[:, part]
        d_mq = (d_mq + nn(mk_t, ds_t, HIGH)) * share
        d_mk = (d_mk + nt(mq_t, ds_t, HIGH)) * share
        dq_ref[part, :] = (d_query + exact_left(d_mq, member)).astype(BF)
        dk_ref[part, :] = (d_keys + exact_left(d_mk, member)).astype(BF)
        d_values = d_values + convolve(d_mixed, row_ref[h], padded) * valid
        dv_ref[part, :] = d_values.astype(BF)
        masked = v * low_valid
        padded[:, MARGIN : MARGIN + slots] = masked
        step = 128
        total = tn(
            jnp.concatenate([d_mixed[:, b * step : (b + 1) * step] for b in range(slots // step)], axis=0),
            jnp.concatenate([padded[:, b * step : (b + 3) * step] for b in range(slots // step)], axis=0),
        )
        high, rest = split(total)
        turned = pltpu.roll(nn(turn, high) + nn(turn, rest), 0, 1, stride=1, stride_axis=0)
        taps_ref[h] = jnp.sum(turned, axis=0, keepdims=True)


def membership(length, slots, turned):
    dims = (slots, LANDMARKS) if turned else (LANDMARKS, slots)
    mark = lax.broadcasted_iota(jnp.int32, dims, 1 if turned else 0)
    position = lax.broadcasted_iota(jnp.int32, dims, 0 if turned else 1)
    low_end = position * LANDMARKS >= mark * length
    high_end = position * LANDMARKS < (mark + 1) * length
    inside = jnp.logical_and(jnp.logical_and(low_end, high_end), position < length)
    return inside.astype(F32)


def tap_rows(taps, reverse):
    taps = taps if reverse else taps[:, ::-1]
    start = 2 * BLOCK - MARGIN - KERNEL // 2
    rows = jnp.pad(taps, ((0, 0), (start, 2 * BLOCK - start - KERNEL)))
    return rows[:, None, :]


def specs(slots):
    big = pl.BlockSpec((2 * HEAD_DIM, slots), lambda i: (i, 0))
    thin = pl.BlockSpec((2 * HEAD_DIM, LANDMARKS), lambda i: (i, 0))
    side = pl.BlockSpec((LANDMARKS, 2 * LANDMARKS), lambda i: (0, i))
    return big, thin, side


def fixed(shape):
    return pl.BlockSpec(shape, lambda i: (0,) * len(shape))


def call(kernel, grid, in_specs, out_specs, out_shape, name, scratch=(), cost=None):
    return pl.pallas_call(
        kernel,
        grid=grid,
        in_specs=in_specs,
        out_specs=out_specs,
        out_shape=out_shape,
        scratch_shapes=list(scratch),
        name=name,
        compiler_params=pltpu.CompilerParams(vmem_limit_bytes=60 * 1024 * 1024),
        cost_estimate=cost,
    )


def shape(dims, kind=F32):
    return jax.ShapeDtypeStruct(dims, kind)


def cost_of(flops, moved):
    return pl.CostEstimate(flops=int(flops), bytes_accessed=int(moved), transcendentals=0)


def ahead(left, right):
    return jnp.dot(left, right, preferred_element_type=jnp.float32)


def against(left, right):
    return lax.dot_general(
        left, right, (((1,), (1,)), ((), ())), preferred_element_type=jnp.float32
    )


def across(left, right):
    return lax.dot_general(
        left, right, (((0,), (0,)), ((), ())), preferred_element_type=jnp.float32
    )


def crossed(left, right):
    return lax.dot_general(
        left, right, (((0,), (1,)), ((), ())), preferred_element_type=jnp.float32
    )


def low(values):
    return values.astype(jnp.bfloat16)


def wide(values):
    return values.astype(jnp.float32)


def layer_norm(values, gain, bias):
    middle = jnp.mean(values, axis=-1, keepdims=True)
    centered = values - middle
    variance = jnp.mean(centered * centered, axis=-1, keepdims=True)
    return centered * lax.rsqrt(variance + 1e-05) * gain + bias


def exact_gelu(values):
    return jax.nn.gelu(values, approximate=False)


def partner(values):
    size = lax.axis_size("mp")
    return lax.ppermute(values, "mp", [(i, (i + 1) % size) for i in range(size)])


def bits_of(size):
    return max(size - 1, 0).bit_length()


def scatter_orders(count):
    if count < 4:
        return [list(range(count))] * 6
    x, y, near, far = [0], [1], [2], list(range(3, count))
    return [
        far + y + x + near, y + far + x + near, x + y + far + near,
        near + x + y + far, x + near + y + far, y + x + near + far,
    ]


def colored(widths, orders):
    streams, turn = [], 0
    for piece, columns in enumerate(widths):
        tiles = columns // 128
        if tiles >= 12:
            chosen = orders
        elif tiles >= 3:
            chosen, turn = orders[3 * turn : 3 * turn + 3], 1 - turn
        else:
            chosen = orders[:1]
        cuts = [round(tiles * part / len(chosen)) * 128 for part in range(len(chosen))] + [columns]
        for low_edge, high_edge, order in zip(cuts[:-1], cuts[1:], chosen):
            if high_edge > low_edge:
                streams.append((piece, low_edge, high_edge, order))
    return streams


def neighbours(count):
    group = lax.axis_index("dp")
    mine = [(group // 2**b) % 2 for b in range(count)]
    return group, mine, [group + (1 - 2 * mine[b]) * 2**b for b in range(count)]


def enter(group, across_bits, core):
    barrier = pltpu.get_barrier_semaphore()
    for other in across_bits:
        pl.semaphore_signal(
            barrier, inc=1, device_id=(other, core), device_id_type=pl.DeviceIdType.MESH
        )
    pl.semaphore_signal(
        barrier, inc=1, device_id=(group, 1 - core), device_id_type=pl.DeviceIdType.MESH
    )
    pl.semaphore_wait(barrier, len(across_bits) + 1)


def remote(source, target, send, arrive, device):
    return pltpu.make_async_remote_copy(
        src_ref=source,
        dst_ref=target,
        send_sem=send,
        recv_sem=arrive,
        device_id=device,
        device_id_type=pl.DeviceIdType.MESH,
    )


def gather_kernel(count, streams, partial, whole, *refs):
    pieces = whole + len(partial)
    blocks, refs = refs[:pieces], refs[pieces:]
    owns, refs = refs[:whole], refs[whole:]
    others, refs = refs[:whole], refs[whole:]
    parts, refs = refs[: len(partial)], refs[len(partial) :]
    send, arrive, side_send, side_arrive, first_send, first_arrive, local = refs
    group, mine, across_bits = neighbours(count)
    core = lax.axis_index("mp")
    twin = (group, 1 - core)

    def view(ref, chosen, columns):
        place = tuple(chosen[b] for b in sorted(chosen, reverse=True))
        return ref.at[place + (slice(None), columns)]

    def own_view(index, chosen):
        piece, low_edge, high_edge, order = streams[index]
        columns = slice(low_edge, high_edge)
        if piece < whole:
            return view(owns[piece], chosen, columns)
        return view(parts[piece - whole], {b: chosen[b] for b in order}, columns)

    def hop(index, place):
        piece, low_edge, high_edge, order = streams[index]
        chosen = {b: slice(None) if b in order[:place] else mine[b] for b in range(count)}
        target = own_view(index, chosen)
        source = blocks[piece].at[:, slice(low_edge, high_edge)] if place == 0 else target
        return remote(
            source, target, send.at[index, place], arrive.at[index, place],
            (across_bits[order[place]], core),
        )

    def forward(index, place):
        piece, low_edge, high_edge, order = streams[index]
        chosen = {b: slice(None) if b in order[:place] else mine[b] for b in range(count)}
        chosen[order[place]] = 1 - mine[order[place]]
        columns = slice(low_edge, high_edge)
        return remote(
            view(owns[piece], chosen, columns), view(others[piece], chosen, columns),
            side_send.at[index, place], side_arrive.at[index, place], twin,
        )

    place_of = {b: mine[b] for b in range(count)}
    enter(group, across_bits, core)
    full = [index for index, stream in enumerate(streams) if stream[0] < whole]
    thin = [index for index, stream in enumerate(streams) if stream[0] >= whole]
    copies, sides = [], []
    hops = {}
    for index in full:
        hops[index] = hop(index, 0)
        hops[index].start()
    for p in range(whole):
        copy = pltpu.make_async_copy(
            blocks[p], view(owns[p], place_of, slice(None)), local.at[p]
        )
        copy.start()
        copies.append(copy)
        side = remote(
            blocks[p], view(others[p], place_of, slice(None)), first_send.at[p],
            first_arrive.at[p], twin,
        )
        side.start()
        sides.append(side)
    lasts = []
    for index in thin:
        piece, low_edge, high_edge, order = streams[index]
        copy = pltpu.make_async_copy(
            blocks[piece].at[:, slice(low_edge, high_edge)], own_view(index, place_of),
            local.at[whole + index - len(full)],
        )
        copy.start()
        lasts.append(copy)
    for copy in copies:
        copy.wait()
    sent = []

    def advance(index, place, places):
        hops[index].wait_recv()
        sent.append(hops[index])
        if place + 1 < places:
            hops[index] = hop(index, place + 1)
            hops[index].start()

    for place in range(count):
        for index in full:
            advance(index, place, count)
            side = forward(index, place)
            side.start()
            sides.append(side)
        if place == count - 3:
            for index in thin:
                hops[index] = hop(index, 0)
                hops[index].start()
            for copy in lasts:
                copy.wait()
        if place == count - 2:
            for step in range(count - 2):
                if step + 1 < count - 2:
                    for index in thin:
                        advance(index, step, count - 2)
    for index in thin:
        advance(index, count - 3, count - 2)
    for one in sent:
        one.wait_send()
    for side in sides:
        side.wait()


def gather_streams(blocks, count, first):
    orders = [order[::-1] for order in scatter_orders(count)]
    return [
        (piece + first, low_edge, high_edge, order)
        for piece, low_edge, high_edge, order in colored([b.shape[1] for b in blocks], orders)
    ]


def gather(blocks, partial, identity):
    groups = lax.axis_size("dp")
    count = bits_of(groups)
    streams = gather_streams(blocks, count, 0)
    full = len(streams)
    streams += [
        (piece, low_edge, high_edge, order[: count - 2])
        for piece, low_edge, high_edge, order in gather_streams(partial, count, len(blocks))
    ]
    results = [jax.ShapeDtypeStruct((2,) * count + b.shape, b.dtype) for b in blocks] * 2
    results += [jax.ShapeDtypeStruct((2,) * (count - 2) + b.shape, b.dtype) for b in partial]
    dma = pltpu.SemaphoreType.DMA
    anywhere = pl.BlockSpec(memory_space=pl.ANY)
    outs = pl.pallas_call(
        functools.partial(gather_kernel, count, streams, partial, len(blocks)),
        in_specs=[pl.BlockSpec(memory_space=pltpu.VMEM)] * (len(blocks) + len(partial)),
        out_specs=[anywhere] * len(results),
        out_shape=results,
        scratch_shapes=[dma((len(streams), count))] * 2
        + [dma((full, count))] * 2
        + [dma((len(blocks),))] * 2
        + [dma((len(blocks) + len(streams) - full,))],
        name="gather",
        compiler_params=pltpu.CompilerParams(collective_id=identity, has_side_effects=True),
    )(*blocks, *partial)
    whole = len(blocks)
    flat = [o.reshape((groups,) + o.shape[count:]) for o in outs[: 2 * whole]]
    return list(zip(flat[:whole], flat[whole:])), outs[2 * whole :]


def lead_kernel(count, streams, groups, pieces, *refs):
    (tokens_ref, lengths_ref, row_ref), refs = refs[:3], refs[3:]
    own_weights, other_weights, refs = refs[:3], refs[3:6], refs[6:]
    parts, refs = refs[:pieces], refs[pieces:]
    (
        q_ref, k_ref, v_ref, out_ref, first_ref, third_ref, summary_ref, carried_ref, mq_ref, mk_ref, a_ref, at_ref,
        z_ref, kept_ref, tokens_t_ref, member_ref, share_ref, valid_ref,
    ), refs = refs[:18], refs[18:]
    owns, refs = refs[:pieces], refs[pieces:]
    others, refs = refs[:pieces], refs[pieces:]
    held, refs = refs[:pieces], refs[pieces:]
    start_ref, padded, member_t_ref, send, arrive, side_send, side_arrive, local, loaded = refs
    step = pl.program_id(0)
    pairs = (pl.num_programs(0) - 1) // 2
    group, mine, across_bits = neighbours(count)
    core = lax.axis_index("mp")
    twin = (group, 1 - core)

    def view(ref, chosen, columns):
        place = tuple(chosen[b] for b in sorted(chosen, reverse=True))
        return ref.at[place + (slice(None), columns)]

    def part_view(index):
        piece, low_edge, high_edge, order = streams[index]
        done = {b: slice(None) for b in order[:-2]}
        return view(parts[piece], done, slice(low_edge, high_edge))

    def placed(ref, index, place, received):
        piece, low_edge, high_edge, order = streams[index]
        chosen = {b: slice(None) if b in order[:place] else mine[b] for b in range(count)}
        if received:
            chosen[order[place]] = 1 - mine[order[place]]
        return view(ref, chosen, slice(low_edge, high_edge))

    def hop(index, turn):
        piece, low_edge, high_edge, order = streams[index]
        place = count - 2 + turn
        target = placed(owns[piece], index, place, False)
        source = part_view(index) if turn == 0 else target
        return remote(
            source, target, send.at[index, turn], arrive.at[index, turn],
            (across_bits[order[place]], core),
        )

    def load(piece):
        return pltpu.make_async_copy(parts[piece], held[piece], loaded.at[piece])

    def settle(index):
        piece, low_edge, high_edge, order = streams[index]
        done = {b: slice(None) for b in order[:-2]}
        return pltpu.make_async_copy(
            view(held[piece], done, slice(low_edge, high_edge)), placed(owns[piece], index, count - 2, False), local.at[index]
        )

    def forward(index, turn):
        piece = streams[index][0]
        if turn == 0:
            source = part_view(index)
            target = placed(others[piece], index, count - 2, False)
        else:
            source = placed(owns[piece], index, count - 3 + turn, True)
            target = placed(others[piece], index, count - 3 + turn, True)
        return remote(
            source, target, side_send.at[index, turn], side_arrive.at[index, turn], twin
        )

    everyone = range(len(streams))

    @pl.when(step == 0)
    def _():
        enter(group, across_bits, core)
        for index in everyone:
            hop(index, 0).start()
        for piece in range(pieces):
            load(piece).start()
        for index in everyone:
            forward(index, 0).start()
        slots = valid_ref.shape[1]
        length = lengths_ref[group * lax.axis_size("mp") + core]
        member_ref[...] = membership(length, slots, False).astype(BF)
        member_t = membership(length, slots, True)
        member_t_ref[...] = member_t.astype(BF)
        share_ref[...] = 1.0 / jnp.sum(member_t, axis=0, keepdims=True)
        valid_ref[...] = (lax.broadcasted_iota(jnp.int32, (1, slots), 1) < length).astype(F32)
        tokens_t_ref[...] = tokens_ref[...].T

    @pl.when(step == 1)
    def _():
        for piece in range(pieces):
            load(piece).wait()
        for index in everyone:
            settle(index).start()

    @pl.when(step == GATHER_WHEN[0])
    def _():
        for index in everyone:
            settle(index).wait()
        for index in everyone:
            hop(index, 0).wait_recv()
            hop(index, 1).start()
            forward(index, 1).start()

    @pl.when(step == GATHER_WHEN[1])
    def _():
        for index in everyone:
            hop(index, 1).wait_recv()
            forward(index, 2).start()

    def project(weights, place):
        side = pl.ds(pl.multiple_of(step * 2 * HEAD_DIM, 2 * HEAD_DIM), 2 * HEAD_DIM)
        columns = pl.ds(pl.multiple_of(place * 2 * HEAD_DIM, 2 * HEAD_DIM), 2 * HEAD_DIM)
        for weight, ref in zip(weights, (q_ref, k_ref, v_ref)):
            ref[side, :] = tn(weight[:, columns], tokens_t_ref[...]).astype(BF)

    @pl.when(step < pairs // 2)
    def _():
        project(own_weights, step)

    @pl.when(jnp.logical_and(step >= pairs // 2, step < pairs))
    def _():
        project(other_weights, step - pairs // 2)

    @pl.when(step < pairs)
    def _():
        side = pl.ds(pl.multiple_of(step * 2 * HEAD_DIM, 2 * HEAD_DIM), 2 * HEAD_DIM)
        marks_kernel(
            q_ref.at[side, :], k_ref.at[side, :], member_t_ref, share_ref, mq_ref.at[side, :], mk_ref.at[side, :],
            a_ref.at[:, side], at_ref.at[:, side], start_ref.at[:, side],
        )

    @pl.when(step == pairs)
    def _():
        inverse_kernel(groups, a_ref, start_ref, z_ref, kept_ref)

    @pl.when(step > pairs)
    def _():
        place = step - pairs - 1
        side = pl.ds(pl.multiple_of(place * 2 * HEAD_DIM, 2 * HEAD_DIM), 2 * HEAD_DIM)
        forward_kernel(
            q_ref.at[side, :], k_ref.at[side, :], v_ref.at[side, :], mq_ref.at[side, :], mk_ref.at[side, :], z_ref.at[:, side],
            valid_ref, row_ref, out_ref, first_ref, third_ref, summary_ref, carried_ref, padded,
        )

    @pl.when(step == 2 * pairs)
    def _():
        for index in everyone:
            for turn in range(2):
                hop(index, turn).wait_send()
            for turn in range(3):
                forward(index, turn).wait()


def attention_lead(tokens, own_weights, other_weights, taps, lengths, parts, identity):
    slots, width = tokens.shape
    pairs = width // (2 * HEAD_DIM)
    groups = width // (4 * HEAD_DIM)
    flat, tall = (LANDMARKS, width), (width, LANDMARKS)
    count = bits_of(lax.axis_size("dp"))
    blocks = [jax.ShapeDtypeStruct(p.shape[count - 2 :], p.dtype) for p in parts]
    streams = gather_streams(blocks, count, 0)
    turns = pairs + 1

    def late(i):
        return i // turns * (i % turns)

    def rows(dims, pick):
        return pl.BlockSpec(dims, lambda i: (pick(i), 0))

    big, thin = (2 * HEAD_DIM, slots), (2 * HEAD_DIM, LANDMARKS)
    anywhere = pl.BlockSpec(memory_space=pl.ANY)
    once = pl.BlockSpec(memory_space=pltpu.VMEM)
    dma = pltpu.SemaphoreType.DMA
    gathered = [shape((2,) * count + b.shape, b.dtype) for b in blocks] * 2
    outs = pl.pallas_call(
        functools.partial(lead_kernel, count, streams, groups, len(parts)),
        grid=(2 * pairs + 1,),
        in_specs=[once, pl.BlockSpec(memory_space=pltpu.SMEM)]
        + [pl.BlockSpec((2, 1, 2 * BLOCK), lambda i: (late(i), 0, 0))]
        + [once] * 6
        + [anywhere] * len(parts),
        out_specs=[once] * 3
        + [rows(big, late)] * 3
        + [rows(thin, late)] * 2
        + [once] * 10
        + [anywhere] * len(gathered),
        out_shape=[shape((width, slots), BF)] * 4
        + [shape((width, slots))] * 2
        + [shape(tall)] * 4
        + [shape(flat)] * 3
        + [
            shape((PINV_STEPS, 4) + flat), shape((width, slots), BF), shape((LANDMARKS, slots), BF),
            shape((1, LANDMARKS)), shape((1, slots)),
        ]
        + gathered,
        scratch_shapes=[pltpu.VMEM(p.shape, p.dtype) for p in parts]
        + [pltpu.VMEM(flat, F32), pltpu.VMEM((HEAD_DIM, slots + MARGIN + BLOCK), BF)]
        + [pltpu.VMEM((slots, LANDMARKS), BF)]
        + [dma((len(streams), 2))] * 2
        + [dma((len(streams), 3))] * 2
        + [dma((len(streams),)), dma((len(parts),))],
        name="lead",
        compiler_params=pltpu.CompilerParams(
            collective_id=identity, has_side_effects=True, vmem_limit_bytes=62 * 1024 * 1024
        ),
        cost_estimate=cost_of(2e10, 3e7),
    )(
        tokens, lengths, tap_rows(taps, False), *own_weights, *other_weights, *parts,
    )
    q, k, v, out, first, third, summary, carried, mq, mk, a, at, z, kept = outs[:14]
    flat_outs = [o.reshape((-1,) + o.shape[count:]) for o in outs[18:]]
    pieces = list(zip(flat_outs[: len(parts)], flat_outs[len(parts) :]))
    saved = (mq, mk, a, at, z, kept, first, third, summary, carried)
    return (q, k, v), out, saved, outs[14:18], pieces


def halving(streams, bits, sums, inbox, send, arrive, across_bits, mine, core, sources=None):
    def columns_of(index):
        return (slice(None), slice(streams[index][1], streams[index][2]))

    def hop(index, place):
        piece, low_edge, high_edge, order = streams[index]
        chosen = {b: mine[b] if b in order[:place] else slice(None) for b in bits[index]}
        chosen[order[place]] = 1 - mine[order[place]]
        held = sources if sources is not None and place == 0 else sums
        source = held[piece].at[tuple(chosen[b] for b in bits[index][::-1]) + columns_of(index)]
        box = inbox[piece][place]
        lead = (slice(None),) * (len(bits[index]) - 1 - place)
        return remote(
            source, box.at[lead + columns_of(index)], send.at[index, place],
            arrive.at[index, place], (across_bits[order[place]], core),
        )

    def add(index, place, half, box):
        piece, low_edge, high_edge, order = streams[index]
        columns = columns_of(index)
        names = bits[index][::-1]
        left = [b for b in bits[index] if b not in order[: place + 1]]
        turn = mine[order[place]] if half else 1 - mine[order[place]]

        def body(i, carry):
            at = {b: mine[b] for b in names}
            at[order[place]] = turn
            for spot, b in enumerate(left):
                at[b] = (i // 2**spot) % 2
            here = tuple(at[b] for b in names)
            there = tuple(at[b] for b in names if b not in order[:place])
            there = here if len(box.shape) == len(here) + 2 else there
            value = sums[piece][here + columns].astype(F32) + box[there + columns].astype(F32)
            sums[piece][here + columns] = value.astype(BF)
            return carry

        lax.fori_loop(0, 2 ** len(left), body, 0)

    return hop, add


def scatter_kernel(count, streams, bits, joined, settled, *refs):
    pieces = len(joined)
    depth = {stream[0]: len(bits[index]) for index, stream in enumerate(streams)}
    owns, refs = refs[:pieces], refs[pieces:]
    others, refs = refs[:pieces], refs[pieces:]
    small_ref, refs = refs[0], refs[1:]
    grads, refs = refs[:3], refs[3:]
    weights, refs = refs[:6], refs[6:]
    results, refs = refs[:pieces], refs[pieces:]
    (total_ref, back_ref), refs = refs[:2], refs[2:]
    sums, refs = refs[:pieces], refs[pieces:]
    twins, refs = refs[:pieces], refs[pieces:]
    inbox = []
    for piece in range(pieces):
        inbox.append(refs[: depth[piece]])
        refs = refs[depth[piece] :]
    small_sum, small_in, send, arrive, side_send, side_arrive, local, small_send, small_arrive = refs
    group, mine, across_bits = neighbours(count)
    core = lax.axis_index("mp")
    twin = (group, 1 - core)
    hop, add = halving(streams, bits, sums, inbox, send, arrive, across_bits, mine, core)
    enter(group, across_bits, core)

    def small_hop(place):
        if place == 0:
            return remote(small_ref, small_in.at[0], small_send.at[0], small_arrive.at[0], twin)
        return remote(
            small_sum.at[place - 1], small_in.at[place], small_send.at[place],
            small_arrive.at[place], (across_bits[place - 1], core),
        )

    small = [small_hop(0)]
    small[0].start()
    starts = []
    for index, (piece, low_edge, high_edge, order) in enumerate(streams):
        lead, tail = (slice(None),) * len(bits[index]), (slice(None), slice(low_edge, high_edge))
        place = lead + tail
        own_place = other_place = place
        if joined[piece] == "rows":
            own_place, other_place = lead + (core,) + tail, lead + (1 - core,) + tail
        if joined[piece] == "columns":
            size = owns[piece].shape[-1] // 2
            other_place = lead + (slice(None), slice(size + low_edge, size + high_edge))
        copy = pltpu.make_async_copy(
            owns[piece].at[own_place], sums[piece].at[place], local.at[index]
        )
        copy.start()
        side = None
        if not settled[piece]:
            side = remote(
                others[piece].at[other_place], twins[piece].at[place], side_send.at[index],
                side_arrive.at[index], twin,
            )
            side.start()
        starts.append((copy, side))

    def back(first, last):
        size = weights[0].shape[1]
        for tile in range(first, last):
            rows = slice(tile * 128, (tile + 1) * 128)
            total = jnp.zeros((128, back_ref.shape[0]), F32)
            for i, weight in enumerate(weights):
                half = slice(i // 3 * size, (i // 3 + 1) * size)
                total = total + nn(weight[rows, :], grads[i % 3][half, :])
            back_ref[:, rows] = total.T

    tiles = back_ref.shape[1] // 128
    hops = [[] for stream in streams]
    for place in range(count):
        back(tiles * place // (count + 1), tiles * (place + 1) // (count + 1))
        small[place].wait_recv()
        before = small_ref[...] if place == 0 else small_sum[place - 1]
        small_sum[place] = before + small_in[place]
        small.append(small_hop(place + 1))
        small[place + 1].start()
        for index, (piece, low_edge, high_edge, order) in enumerate(streams):
            if place >= len(order):
                continue
            box = twins[piece] if place == 0 else inbox[piece][place - 1]
            if place == 0:
                copy, side = starts[index]
                copy.wait()
                if side is not None:
                    side.wait_recv()
            else:
                hops[index][place - 1].wait_recv()
            if place > 0 or side is not None:
                add(index, place, 0, box)
            one = hop(index, place)
            one.start()
            hops[index].append(one)
            if place > 0 or side is not None:
                add(index, place, 1, box)
    back(tiles * count // (count + 1), tiles)
    small[count].wait_recv()
    total_ref[...] = small_sum[count - 1] + small_in[count]
    for index, (piece, low_edge, high_edge, order) in enumerate(streams):
        hops[index][-1].wait_recv()
        columns = (slice(None), slice(low_edge, high_edge))
        results[piece][columns] = (
            sums[piece][tuple(mine[b] for b in bits[index][::-1]) + columns].astype(F32)
            + inbox[piece][-1][columns].astype(F32)
        )
    for copy, side in starts:
        if side is not None:
            side.wait_send()
    for one in small:
        one.wait_send()
    for line in hops:
        for one in line:
            one.wait_send()


def scatter(owns, others, small, grads, weights, identity):
    groups = lax.axis_size("dp")
    count = bits_of(groups)
    settled = [other is None for other in others]
    joined = [
        "rows" if own.ndim == 4 else "columns" if own is other else ""
        for own, other in zip(owns, others)
    ]
    shapes = [
        (b.shape[-2], b.shape[-1] // 2 if how == "columns" else b.shape[-1])
        for b, how in zip(owns, joined)
    ]
    depths = [bits_of(b.shape[0]) for b in owns]
    streams = [
        (piece, low_edge, high_edge, order[count - depths[piece] :])
        for piece, low_edge, high_edge, order in colored(
            [dims[-1] for dims in shapes], scatter_orders(count)
        )
    ]
    bits = [sorted(stream[3]) for stream in streams]
    leads = [(2,) * depth for depth in depths]
    dma = pltpu.SemaphoreType.DMA
    vmem = pl.BlockSpec(memory_space=pltpu.VMEM)
    others = [own if other is None else other for own, other in zip(owns, others)]
    outs = pl.pallas_call(
        functools.partial(scatter_kernel, count, streams, bits, joined, settled),
        in_specs=[pl.BlockSpec(memory_space=pl.ANY)] * (2 * len(owns)) + [vmem] * 10,
        out_specs=[vmem] * (len(owns) + 2),
        out_shape=[jax.ShapeDtypeStruct(s, F32) for s in shapes]
        + [
            jax.ShapeDtypeStruct(small.shape, F32),
            jax.ShapeDtypeStruct((grads[0].shape[1], weights[0].shape[0]), F32),
        ],
        scratch_shapes=[pltpu.VMEM(lead + s, BF) for lead, s in zip(leads, shapes)]
        + [
            pltpu.VMEM((8, 128) if done else lead + s, BF)
            for lead, s, done in zip(leads, shapes, settled)
        ]
        + [
            pltpu.VMEM(lead[: len(lead) - 1 - place] + s, BF)
            for lead, s in zip(leads, shapes)
            for place in range(len(lead))
        ]
        + [pltpu.VMEM((count,) + small.shape, F32), pltpu.VMEM((count + 1,) + small.shape, F32)]
        + [dma((len(streams), count))] * 2
        + [dma((len(streams),))] * 3
        + [dma((count + 1,))] * 2,
        name="scatter",
        compiler_params=pltpu.CompilerParams(
            collective_id=identity, has_side_effects=True, vmem_limit_bytes=62 * 1024 * 1024
        ),
    )(
        *[
            b.reshape(lead + b.shape[1:])
            for b, lead in zip(owns + others, leads + leads)
        ],
        small,
        *grads,
        *weights,
    )
    return outs[:-2], outs[-2], outs[-1]


def tail_kernel(count, streams, bits, groups, pieces, *refs):
    (
        d_ref, q_ref, k_ref, v_ref, first_ref, third_ref, mq_ref, mk_ref, carried_ref, a_ref,
        at_ref, z_ref, kept_ref, summary_ref, member_ref, share_ref, valid_ref, row_ref, tokens_ref,
    ), refs = refs[:19], refs[19:]
    sources, refs = refs[:pieces], refs[pieces:]
    (dq_ref, dk_ref, dv_ref, taps_ref), refs = refs[:4], refs[4:]
    weight_grads, refs = refs[:3], refs[3:]
    results, refs = refs[:pieces], refs[pieces:]
    (gz_ref, dsum_ref, ds_ref, padded), refs = refs[:4], refs[4:]
    sums, refs = refs[:pieces], refs[pieces:]
    hop_count = len(streams[0][3])
    inbox = []
    for piece in range(pieces):
        inbox.append(refs[:hop_count])
        refs = refs[hop_count:]
    send, arrive, local, store = refs
    step = pl.program_id(0)
    pairs = (pl.num_programs(0) - 1) // 2
    group, mine, across_bits = neighbours(count)
    core = lax.axis_index("mp")
    hop, add = halving(
        streams, bits, sums, inbox, send, arrive, across_bits, mine, core, sources
    )

    def load(piece):
        return pltpu.make_async_copy(sources[piece], sums[piece], local.at[piece])

    def save(index):
        piece, low_edge, high_edge, order = streams[index]
        columns = (slice(None), slice(low_edge, high_edge))
        spot = tuple(slice(None) if b not in order else mine[b] for b in bits[index][::-1])
        lead = (slice(None),) * (count - hop_count)
        return pltpu.make_async_copy(
            sums[piece].at[spot + columns], results[piece].at[lead + columns], store.at[index]
        )

    @pl.when(step == 0)
    def _():
        enter(group, across_bits, core)
        for index in range(len(streams)):
            hop(index, 0).start()
        for piece in range(pieces):
            load(piece).start()

    def add_last(index, box):
        piece, low_edge, high_edge, order = streams[index]
        columns = (slice(None), slice(low_edge, high_edge))
        left = [b for b in bits[index] if b not in order]

        def body(i, carry):
            at = {b: mine[b] for b in bits[index]}
            for spot, b in enumerate(left):
                at[b] = (i // 2**spot) % 2
            here = tuple(at[b] for b in bits[index][::-1])
            there = tuple(at[b] for b in bits[index][::-1] if b in left)
            value = sums[piece][here + columns].astype(F32) + box[there + columns].astype(F32)
            sums[piece][here + columns] = value.astype(BF)
            return carry

        lax.fori_loop(0, 2 ** len(left), body, 0)

    for place in range(1, hop_count + 1):

        @pl.when(step == WHEN[place])
        def _():
            if place == 1:
                for piece in range(pieces):
                    load(piece).wait()
            for index, (piece, low_edge, high_edge, order) in enumerate(streams):
                hop(index, place - 1).wait_recv()
                box = inbox[piece][place - 1]
                if place < hop_count:
                    add(index, place, 0, box)
                    hop(index, place).start()
                    add(index, place, 1, box)
                else:
                    add_last(index, box)

    @pl.when(step < pairs)
    def _():
        side = pl.ds(pl.multiple_of(step * 2 * HEAD_DIM, 2 * HEAD_DIM), 2 * HEAD_DIM)
        carried_back_kernel(
            d_ref, first_ref, z_ref, summary_ref, valid_ref, gz_ref.at[:, side],
            dsum_ref.at[side, :],
        )

    @pl.when(step == pairs)
    def _():
        inverse_back_kernel(groups, a_ref, at_ref, kept_ref, gz_ref, ds_ref)

    @pl.when(step > pairs)
    def _():
        place = step - pairs - 1
        side = pl.ds(pl.multiple_of(place * 2 * HEAD_DIM, 2 * HEAD_DIM), 2 * HEAD_DIM)
        backward_kernel(
            d_ref, q_ref, k_ref, v_ref, first_ref, third_ref, mq_ref, mk_ref, carried_ref,
            dsum_ref.at[side, :], ds_ref.at[:, side], member_ref, share_ref, valid_ref, row_ref,
            dq_ref, dk_ref, dv_ref, taps_ref, padded,
        )
        for grad, ref in zip((dq_ref, dk_ref, dv_ref), weight_grads):
            ref[...] = nt(tokens_ref[...], grad[...]).astype(BF)

    @pl.when(step == 2 * pairs)
    def _():
        for index in range(len(streams)):
            save(index).start()
        for index in range(len(streams)):
            for place in range(hop_count):
                hop(index, place).wait_send()
        for index in range(len(streams)):
            save(index).wait()


def attention_tail(d, q, k, v, taps, setup, saved, grads, identity):
    mq, mk, a, at, z, kept, first, third, summary, carried = saved
    width, slots = q.shape
    pairs = width // (2 * HEAD_DIM)
    groups = width // (4 * HEAD_DIM)
    tokens_t, member, share, valid = setup
    flat = (LANDMARKS, width)
    count = bits_of(lax.axis_size("dp"))
    hop_count = min(3, count - 1)
    streams = [
        (piece, low_edge, high_edge, order[:hop_count])
        for piece, low_edge, high_edge, order in colored(
            [b.shape[-1] for b in grads], scatter_orders(count)
        )
    ]
    bits = [list(range(count))] * len(streams)
    lead = (2,) * count
    shapes = [b.shape[1:] for b in grads]
    turns = pairs + 1

    def both(i):
        return i % turns - i % turns // pairs

    def late(i):
        return i // turns * (i % turns)

    def early(i):
        return both(i) * (1 - i // turns) + (pairs - 1) * (i // turns)

    def spec(dims, index):
        return pl.BlockSpec(dims, index)

    big, tall, side = (2 * HEAD_DIM, slots), (2 * HEAD_DIM, LANDMARKS), (LANDMARKS, 2 * LANDMARKS)

    def rows(dims, pick):
        return spec(dims, lambda i: (pick(i), 0))

    anywhere = pl.BlockSpec(memory_space=pl.ANY)
    once = pl.BlockSpec(memory_space=pltpu.VMEM)
    dma = pltpu.SemaphoreType.DMA
    outs = pl.pallas_call(
        functools.partial(tail_kernel, count, streams, bits, groups, len(grads)),
        grid=(2 * pairs + 1,),
        in_specs=[
            rows(big, both), rows(big, late), rows(big, late), rows(big, late), rows(big, both),
            rows(big, late), rows(tall, late), rows(tall, late), rows(tall, late), once, once,
            spec(side, lambda i: (0, early(i))), once, rows(tall, early), once, once, once,
            spec((2, 1, 2 * BLOCK), lambda i: (late(i), 0, 0)), once,
        ]
        + [anywhere] * len(grads),
        out_specs=[rows(big, late)] * 3
        + [spec((2, 1, 384), lambda i: (late(i), 0, 0))]
        + [spec((width, 2 * HEAD_DIM), lambda i: (0, late(i)))] * 3
        + [anywhere] * len(grads),
        out_shape=[shape(q.shape, BF)] * 3
        + [shape((2 * pairs, 1, 384))]
        + [shape((width, width), BF)] * 3
        + [shape((2,) * (count - hop_count) + s, BF) for s in shapes],
        scratch_shapes=[
            pltpu.VMEM(flat, F32), pltpu.VMEM((width, LANDMARKS), F32), pltpu.VMEM(flat, F32),
            pltpu.VMEM((HEAD_DIM, slots + MARGIN + BLOCK), BF),
        ]
        + [pltpu.VMEM(lead + s, BF) for s in shapes]
        + [
            pltpu.VMEM(lead[: count - 1 - place] + s, BF)
            for s in shapes
            for place in range(hop_count)
        ]
        + [dma((len(streams), hop_count))] * 2
        + [dma((len(grads),)), dma((len(streams),))],
        name="tail",
        compiler_params=pltpu.CompilerParams(
            collective_id=identity, has_side_effects=True, vmem_limit_bytes=62 * 1024 * 1024
        ),
        cost_estimate=cost_of(4e10, 4e7),
    )(
        d, q, k, v, first, third, mq, mk, carried, a, at, z, kept, summary, member, share, valid,
        tap_rows(taps, True), tokens_t, *[b.reshape(lead + b.shape[1:]) for b in grads],
    )
    dq, dk, dv, spread = outs[:4]
    sums = [o.reshape((-1,) + s) for o, s in zip(outs[7:], shapes)]
    start = 2 * MARGIN - 1 - KERNEL // 2
    return (dq, dk, dv), spread[:, 0, start : start + KERNEL], outs[4:7], sums


def normed(values):
    centered = values - jnp.mean(values, axis=1, keepdims=True)
    scale = lax.rsqrt(jnp.mean(centered * centered, axis=1, keepdims=True) + 1e-05)
    return centered * scale, scale


def normed_back(grad, unit, scale):
    return scale * (
        grad
        - jnp.mean(grad, axis=1, keepdims=True)
        - unit * jnp.mean(grad * unit, axis=1, keepdims=True)
    )


def middle_kernel(
    chunk, att_ref, tokens_ref, grad_ref, output_ref, e_own_ref, e_oth_ref, s_own_ref, s_oth_ref,
    norms_ref, out_ref, first_in_ref, branch_ref, hidden_ref, act_own_ref, act_oth_ref,
    pre_own_ref, pre_oth_ref, projected_ref, attended_ref, small_ref, slope_ref,
):
    gain_one, bias_one, gain_two, bias_two = (norms_ref[i : i + 1, :] for i in range(4))
    projected = nn(output_ref[...], att_ref[...]).T
    unit_one, scale_one = normed(tokens_ref[...].astype(F32) + projected)
    first_out = unit_one * gain_one + bias_one
    hidden_in = first_out.astype(BF)
    hidden_ref[...] = hidden_in
    size = e_own_ref.shape[1]
    total = first_out
    sides = ((e_own_ref, s_own_ref, act_own_ref), (e_oth_ref, s_oth_ref, act_oth_ref))
    for side, (e_ref, s_ref, act_ref) in enumerate(sides):
        for start in range(0, size, chunk):
            part = slice(start, start + chunk)
            pre = nn(hidden_in, e_ref[:, part])
            share = 0.5 * (1.0 + lax.erf(pre * 0.7071067811865476))
            density = jnp.exp(-0.5 * pre * pre) * 0.3989422804014327
            active = (pre * share).astype(BF)
            act_ref[:, part] = active
            slope_ref[:, side * size + start : side * size + start + chunk] = (
                share + pre * density
            )
            total = total + nt(active, s_ref[:, part])
    unit_two, scale_two = normed(total)
    out_ref[...] = (unit_two * gain_two + bias_two).astype(BF)
    grad = grad_ref[...].astype(F32)
    second_in = normed_back(grad * gain_two, unit_two, scale_two)
    d_branch = second_in.astype(BF)
    branch_ref[...] = d_branch
    first_grad = second_in
    sides = ((e_own_ref, s_own_ref, pre_own_ref), (e_oth_ref, s_oth_ref, pre_oth_ref))
    for side, (e_ref, s_ref, pre_ref) in enumerate(sides):
        for start in range(0, size, chunk):
            part = slice(start, start + chunk)
            d_pre = (
                nn(d_branch, s_ref[:, part])
                * slope_ref[:, side * size + start : side * size + start + chunk]
            ).astype(BF)
            pre_ref[:, part] = d_pre
            first_grad = first_grad + nt(d_pre, e_ref[:, part])
    first_in = normed_back(first_grad * gain_one, unit_one, scale_one)
    first_in_ref[...] = first_in
    d_projected = first_in.astype(BF)
    projected_ref[...] = d_projected
    attended_ref[...] = nn(d_projected, output_ref[...]).T.astype(BF)
    sums = jnp.concatenate(
        [
            jnp.sum(x, axis=0, keepdims=True)
            for x in (first_grad * unit_one, first_grad, grad * unit_two, grad)
        ],
        axis=0,
    )

    @pl.when(pl.program_id(0) == 0)
    def _():
        small_ref[...] = sums

    @pl.when(pl.program_id(0) > 0)
    def _():
        small_ref[...] += sums


def middle(att, tokens, grad, output_t, e_own, e_oth, s_own, s_oth, norms):
    slots, width = tokens.shape
    size = e_own.shape[1]
    tile = TILE
    once = pl.BlockSpec(memory_space=pltpu.VMEM)

    def rows(columns):
        return pl.BlockSpec((tile, columns), lambda i: (i, 0))

    across_tile = pl.BlockSpec((width, tile), lambda i: (0, i))
    return call(
        functools.partial(middle_kernel, CHUNK if size % CHUNK == 0 else size), (slots // tile,),
        [across_tile, rows(width), rows(width)] + [once] * 6,
        [rows(width)] * 4 + [rows(size)] * 4 + [rows(width), across_tile, fixed((4, width))],
        [
            shape((slots, width), BF), shape((slots, width)), shape((slots, width), BF),
            shape((slots, width), BF),
        ]
        + [shape((slots, size), BF)] * 4
        + [shape((slots, width), BF), shape((width, slots), BF), shape((4, width))],
        "middle", [pltpu.VMEM((tile, 2 * size), F32)], cost=cost_of(2.2e10, 4e7),
    )(att, tokens, grad, output_t, e_own, e_oth, s_own, s_oth, norms)


def on_device(
    tokens,
    w_query,
    w_key,
    w_value,
    value_taps,
    w_output,
    first_gain,
    first_bias,
    w_expand,
    w_shrink,
    second_gain,
    second_bias,
    doc_lengths,
    out_grad,
):
    parts = lax.axis_size("mp")
    groups = lax.axis_size("dp")
    group = lax.axis_index("dp")
    core = lax.axis_index("mp")
    slots, width = tokens.shape
    half = w_query.shape[1]
    hidden_half = w_expand.shape[1]
    rows = w_query.shape[0]

    def in_core_order(own, other, axis):
        return jnp.where(
            core == 0,
            jnp.concatenate([own, other], axis=axis),
            jnp.concatenate([other, own], axis=axis),
        )

    sides = rows // parts
    own_heads = value_taps.shape[0]
    notes = jnp.pad(value_taps, ((8, 8 - own_heads), (0, 128 - KERNEL)))
    for row, norm in enumerate((first_gain, first_bias, second_gain, second_bias)):
        notes = notes + jnp.pad(wide(norm)[None], ((row, 15 - row), (0, 128 - sides)))
    heads, hidden_parts = gather(
        [w_query, w_key, w_value, w_output.T, notes], [w_expand, w_shrink.T], 0
    )
    (out_own, out_other), (note_own, note_other) = heads[3:]
    output_t = in_core_order(out_own[:, None], out_other[:, None], 1).reshape(width, width)
    output_t = jnp.where(
        core == 0, output_t, jnp.concatenate([output_t[:, half:], output_t[:, :half]], axis=1)
    )
    norms = in_core_order(note_own[:, None, :4, :sides], note_other[:, None, :4, :sides], 1)
    norms = norms.transpose(2, 0, 1, 3).reshape(4, width)
    other_taps = lax.dynamic_index_in_dim(note_other, group, 0, keepdims=False)
    taps = jnp.concatenate([value_taps, other_taps[8 : 8 + own_heads, :KERNEL]], axis=0)

    def flat(pair):
        return pair[0].reshape(width, -1), pair[1].reshape(width, -1)

    (q_own, q_oth), (k_own, k_oth), (v_own, v_oth) = (flat(pair) for pair in heads[:3])

    own_weights, other_weights = [q_own, k_own, v_own], [q_oth, k_oth, v_oth]
    (query, keys, values), attended, saved, setup, hiddens = attention_lead(
        tokens, own_weights, other_weights, taps, doc_lengths, hidden_parts, 3
    )
    (e_own, e_oth), (s_own, s_oth) = (flat(pair) for pair in hiddens)
    (
        layer_out, d_first_in, d_branch, hidden_in, act_own, act_oth, d_pre_own, d_pre_oth,
        d_projected, d_attended, norm_sums,
    ) = middle(attended, tokens, out_grad, output_t, e_own, e_oth, s_own, s_oth, norms)

    def blocks(values):
        return low(values).reshape(groups, rows, values.shape[1])

    shrink_got = partner(low(across(d_branch, act_oth)))
    expand_got = partner(low(across(hidden_in, d_pre_oth)))
    shrink_sum = blocks(across(d_branch, act_own) + wide(shrink_got))
    expand_sum = blocks(across(hidden_in, d_pre_own) + wide(expand_got))
    head_grads, taps_grad, weight_grads, (shrink_part, expand_part) = attention_tail(
        d_attended, query, keys, values, taps, setup, saved, [shrink_sum, expand_sum], 2
    )
    output_part = in_core_order(
        low(crossed(d_projected, attended[:half])), low(crossed(d_projected, attended[half:])), 1
    ).reshape(groups, parts, sides, width)
    taps_grad = in_core_order(taps_grad[:own_heads], taps_grad[own_heads:], 0)
    small = jnp.concatenate(
        [
            norm_sums,
            jnp.pad(taps_grad, ((0, 12 - taps_grad.shape[0]), (0, width - KERNEL))),
        ],
        axis=0,
    )
    query_part, keys_part, values_part = (
        grad.reshape(groups, rows, width) for grad in weight_grads
    )
    pieces = [shrink_part, expand_part, query_part, keys_part, values_part, output_part]
    sums, small, back = scatter(
        pieces, [None, None] + pieces[2:], small, head_grads, own_weights + other_weights, 1
    )
    shrink_grad, expand_grad, query_grad, key_grad, value_grad, output_grad = sums
    tokens_grad = d_first_in + back
    taps_grad = lax.dynamic_slice(small, (4 + core * own_heads, 0), (own_heads, KERNEL))
    norm_grads = lax.dynamic_slice(small, (0, group * rows + core * sides), (4, sides))
    return (
        layer_out,
        tokens_grad,
        query_grad,
        key_grad,
        value_grad,
        taps_grad,
        output_grad.T,
        norm_grads[0],
        norm_grads[1],
        expand_grad,
        shrink_grad.T,
        norm_grads[2],
        norm_grads[3],
    )


def solution(mesh):
    tokens_spec = P(("dp", "mp"), None)
    vector = P(("dp", "mp"))
    in_specs = (
        tokens_spec,
        P("dp", "mp"),
        P("dp", "mp"),
        P("dp", "mp"),
        P("mp", None),
        P(None, ("dp", "mp")),
        vector,
        vector,
        P("dp", "mp"),
        P("mp", "dp"),
        vector,
        vector,
        P(),
        tokens_spec,
    )
    out_specs = (
        tokens_spec,
        tokens_spec,
        P("dp", "mp"),
        P("dp", "mp"),
        P("dp", "mp"),
        P("mp", None),
        P(None, ("dp", "mp")),
        vector,
        vector,
        P("dp", "mp"),
        P("mp", "dp"),
        vector,
        vector,
    )
    return jax.shard_map(
        on_device, mesh=mesh, in_specs=in_specs, out_specs=out_specs, check_vma=False
    )
```
